128 devices in a mesh: rows: 64 (over z, y, x), grp: 2 (over core).
Axes of the slice: x: 4, y: 4, z: 4, core: 2. Of those that a mesh axis runs over, the one named last changes fastest.
Arguments:
- earlier: bfloat16 [524288, 1024], P(('rows', 'grp')), may hold values from -6 to 6
- snapshots: bfloat16 [524288, 512], P(('rows', 'grp')), may hold values from -8 to 8
- later: bfloat16 [524288, 512], P(('rows', 'grp')), may hold values from -8 to 8
Outputs:
- basis: bfloat16 [524288, 512], P(('rows', 'grp'))
- factors: float32 [2, 256, 256], replicated
- shift_block: float32 [512, 512], replicated
The draws below stay inside these ranges and needn't reach their ends.
All inputs are finite; a program needn't handle non-finite values.
Results may differ from the reference program's by a relative error of at most 0.0045.
The reference program's roundings to bfloat16 on the way count: a program that leaves them out, or rounds other values in their place, can miss the bound.
Values sent between devices are 32-bit elements; how exact they have to be, the bound alone decides.
A program may use at most 128 MiB of HBM per device.

```python
import jax
import jax.numpy as jnp
from jax import lax

K0 = 1024
PANEL = 256
ROWS = 524288


def make_parts(key):
    space = jax.random.normal(jax.random.fold_in(key, 11), (ROWS, K0), jnp.float32)
    mixing = jax.random.normal(jax.random.fold_in(key, 12), (K0, 2 * PANEL + 1), jnp.float32) / K0 ** 0.5
    noise = jax.random.normal(jax.random.fold_in(key, 13), (ROWS, 2 * PANEL + 1), jnp.float32)
    height = 0.15
    space = jnp.clip(space, -6.0, 6.0)
    position = jnp.arange(ROWS, dtype=jnp.float32) / ROWS
    spread = height * jnp.exp(jnp.log(3.0) * position)
    return (space, mixing, noise, spread)


def draw_earlier(key, part):
    space, mixing, noise, spread = make_parts(key)
    return space.astype(jnp.bfloat16)


def draw_snapshots(key, part):
    space, mixing, noise, spread = make_parts(key)
    fields = jnp.dot(space, mixing[:, :2 * PANEL]) + spread[:, None] * noise[:, :2 * PANEL]
    return jnp.clip(fields, -8.0, 8.0).astype(jnp.bfloat16)


def draw_later(key, part):
    space, mixing, noise, spread = make_parts(key)
    mapping = jax.random.normal(jax.random.fold_in(key, 14), (2 * PANEL, 2 * PANEL), jnp.float32)
    carried = 0.6 * noise[:, 1:] + 0.8 * jnp.dot(noise[:, :2 * PANEL], mapping) / (2 * PANEL) ** 0.5
    fields = jnp.dot(space, mixing[:, 1:]) + spread[:, None] * carried
    return jnp.clip(fields, -8.0, 8.0).astype(jnp.bfloat16)


def setup_inputs(seed: int = 0) -> dict:
    seeds = jax.random.split(jax.random.key(seed), 4)
    earlier = draw_earlier(jax.random.fold_in(seeds[3], 71), 0)
    snapshots = draw_snapshots(jax.random.fold_in(seeds[3], 71), 0)
    later = draw_later(jax.random.fold_in(seeds[3], 71), 0)
    return {"earlier": earlier, "snapshots": snapshots, "later": later}


def inner(left, right):
    return jnp.dot(left.T.astype(jnp.float32), right.astype(jnp.float32), preferred_element_type=jnp.float32) / ROWS

def factor(gram, second):
    lower = jnp.linalg.cholesky(gram)
    inverse = jax.scipy.linalg.solve_triangular(lower, jnp.eye(gram.shape[0], dtype=jnp.float32), lower=True)
    newcols = jnp.dot(second, inverse.T, precision=lax.Precision.HIGHEST).astype(jnp.bfloat16)
    return (newcols, lower.T)

def orthogonalize(space, panel):
    first = inner(space, panel)
    once = (panel.astype(jnp.float32) - jnp.dot(space.astype(jnp.float32), first.astype(jnp.bfloat16).astype(jnp.float32), preferred_element_type=jnp.float32)).astype(jnp.bfloat16)
    second = inner(space, once)
    twice = once.astype(jnp.float32) - jnp.dot(space.astype(jnp.float32), second.astype(jnp.bfloat16).astype(jnp.float32), preferred_element_type=jnp.float32)
    gram = jnp.dot(twice.T, twice, precision=lax.Precision.HIGHEST) / ROWS
    return factor(gram, twice)

def reference(earlier, snapshots, later):
    q_first, r_first = orthogonalize(earlier, snapshots[:, :PANEL])
    space = jnp.concatenate([earlier, q_first], axis=1)
    q_second, r_second = orthogonalize(space, snapshots[:, PANEL:])
    basis = jnp.concatenate([q_first, q_second], axis=1)
    shift_block = inner(basis, later)
    return (basis, jnp.stack([r_first, r_second]), shift_block)
```

```python
import functools
import itertools

import jax
import jax.numpy as jnp
from jax import lax
from jax.experimental import pallas as pl
from jax.experimental.pallas import tpu as pltpu
from jax.sharding import Mesh
from jax.sharding import PartitionSpec as P

PANEL = 256
BLOCK = 32
HALF = 128
AXES = ("rows_0", "rows_1", "rows_2", "grp")


def thirds(value):
    top = value.astype(jnp.bfloat16)
    rest = value - top.astype(jnp.float32)
    middle = rest.astype(jnp.bfloat16)
    low = (rest - middle.astype(jnp.float32)).astype(jnp.bfloat16)
    return top, middle, low


def halves(value):
    top = value.astype(jnp.bfloat16)
    return top, (value - top.astype(jnp.float32)).astype(jnp.bfloat16)


MESH = pl.DeviceIdType.MESH


def offsets(stage):
    sizes = [2 if axis == "grp" else 4 for axis in stage]
    return [o for o in itertools.product(*[range(s) for s in sizes]) if any(o)]


def peer_of(stage, offset):
    return {
        axis: lax.rem(lax.axis_index(axis) + shift, 2 if axis == "grp" else 4)
        for axis, shift in zip(stage, offset)
        if shift
    }


def place_in(stage, offset=None):
    place = 0
    for n, axis in enumerate(stage):
        size = 2 if axis == "grp" else 4
        at = lax.axis_index(axis)
        if offset is not None:
            at = lax.rem(at + offset[n], size)
        place = place * size + at
    return place


def size_of(stage):
    size = 1
    for axis in stage:
        size *= 2 if axis == "grp" else 4
    return size


def sum_kernel(colors, x_ref, o_ref, *scratch):
    it = iter(scratch)
    state = []
    for start, rows, stages in colors:
        levels = []
        length = rows
        for stage in stages:
            length //= size_of(stage)
            levels.append((stage, offsets(stage), length, next(it), next(it), next(it), next(it), next(it), next(it)))
        state.append((start, levels))
    greeted = []
    for _, levels in state:
        for level in levels:
            for offset in level[1]:
                key = tuple(sorted((a, o) for a, o in zip(level[0], offset) if o))
                if key not in greeted:
                    greeted.append(key)
    barrier = pltpu.get_barrier_semaphore()
    for key in greeted:
        pl.semaphore_signal(barrier, inc=1, device_id=peer_of([a for a, _ in key], [o for _, o in key]), device_id_type=MESH)
    pl.semaphore_wait(barrier, len(greeted))

    depth = max(len(levels) for _, levels in state)
    pending = []
    where = [start for start, _ in state]
    live = [None] * len(state)

    def finish(c, s):
        stage, offs, length, slots, acc = state[c][1][s][:5]
        own = pl.multiple_of(place_in(stage) * length, 8)
        for copy in live[c]:
            copy.wait_recv()
        src = x_ref if s == 0 else state[c][1][s - 1][4]
        base = where[c] if s == 0 else 0
        value = src[pl.ds(pl.multiple_of(base + own, 8), length), :]
        for n in range(len(offs)):
            value = value + slots[n]
        where[c] = where[c] + own
        last = s + 1 == len(state[c][1])
        if last:
            o_ref[pl.ds(pl.multiple_of(where[c], 8), length), :] = value
        else:
            acc[...] = value

    for s in range(depth + 1):
        for c, (start, levels) in enumerate(state):
            if s > 0 and s <= len(levels):
                finish(c, s - 1)
            if s < len(levels):
                stage, offs, length, slots, acc, send, recv, _, _ = levels[s]
                src = x_ref if s == 0 else levels[s - 1][4]
                base = start if s == 0 else 0
                live[c] = []
                for n, offset in enumerate(offs):
                    at = pl.multiple_of(base + place_in(stage, offset) * length, 8)
                    copy = pltpu.make_async_remote_copy(
                        src_ref=src.at[pl.ds(at, length), :], dst_ref=slots.at[n],
                        send_sem=send.at[n], recv_sem=recv.at[n],
                        device_id=peer_of(stage, offset), device_id_type=MESH)
                    copy.start()
                    live[c].append(copy)
                    pending.append(copy)
    gath = [None] * len(state)
    for s in range(depth + 1):
        for c, (start, levels) in enumerate(state):
            k = len(levels) - 1 - s
            if s > 0 and s <= len(levels):
                for copy in gath[c]:
                    copy.wait_recv()
                stage, _, length = levels[k + 1][:3]
                where[c] = where[c] - place_in(stage) * length
            if k >= 0:
                stage, offs, length, _, _, _, _, send, recv = levels[k]
                gath[c] = []
                at = pl.multiple_of(where[c], 8)
                for n, offset in enumerate(offs):
                    copy = pltpu.make_async_remote_copy(
                        src_ref=o_ref.at[pl.ds(at, length), :], dst_ref=o_ref.at[pl.ds(at, length), :],
                        send_sem=send.at[n], recv_sem=recv.at[n],
                        device_id=peer_of(stage, offset), device_id_type=MESH)
                    copy.start()
                    gath[c].append(copy)
                    pending.append(copy)
    for copy in pending:
        copy.wait_send()


def summed(x, colors, cid):
    scratch = []
    for start, rows, stages in colors:
        length = rows
        for stage in stages:
            length //= size_of(stage)
            n = size_of(stage) - 1
            assert length % 8 == 0
            scratch += [pltpu.VMEM((n, length, 128), jnp.float32), pltpu.VMEM((length, 128), jnp.float32)]
            scratch += [pltpu.SemaphoreType.DMA((n,))] * 4
    return pl.pallas_call(
        functools.partial(sum_kernel, colors),
        out_shape=jax.ShapeDtypeStruct(x.shape, x.dtype),
        in_specs=[pl.BlockSpec(memory_space=pltpu.VMEM)],
        out_specs=pl.BlockSpec(memory_space=pltpu.VMEM),
        scratch_shapes=scratch,
        compiler_params=pltpu.CompilerParams(collective_id=cid, has_side_effects=True, vmem_limit_bytes=50 * 2**20),
        name="summed%d" % cid,
    )(x)


G, X, Y, Z = "grp", "rows_2", "rows_1", "rows_0"
THREE = [((G,), (X,), (Y,), (Z,)), ((G,), (Y,), (Z,), (X,)), ((G,), (Z,), (X,), (Y,))]
ONE = [((G,), (X, Y, Z))]


def colored(rows, orders):
    each = rows // len(orders)
    return [(n * each, each, order) for n, order in enumerate(orders)]


def factor(work, upper_ref, inverse_ref):
    lane = lax.broadcasted_iota(jnp.int32, (BLOCK, PANEL), 1)
    sub = lax.broadcasted_iota(jnp.int32, (BLOCK, HALF), 0)
    lane_half = lax.broadcasted_iota(jnp.int32, (BLOCK, HALF), 1)
    for k in range(PANEL // BLOCK):
        at = k * BLOCK
        rows = work[at : at + BLOCK, :]
        base = at // HALF * HALF
        off = at - base
        diag = rows[:, base : base + HALF]
        cols = [jnp.broadcast_to(diag[:, off + j : off + j + 1], (BLOCK, HALF)) for j in range(BLOCK)]
        eye = (lane_half == sub + off).astype(jnp.float32)
        wide = [rows[:, :HALF], rows[:, HALF:]]
        own = base // HALF
        inside = (lane_half >= off) & (lane_half < off + BLOCK)
        wide[own] = jnp.where(inside, eye, wide[own])
        scale = jnp.zeros((BLOCK, HALF), jnp.float32)
        for j in range(BLOCK):
            pivot = jnp.broadcast_to(cols[j][j : j + 1, :], (BLOCK, HALF))
            scale = jnp.where(sub == j, pivot, scale)
            if j == BLOCK - 1:
                break
            ratio = cols[j] * (1.0 / pivot)
            ratio = jnp.where(sub > j, ratio, 0.0)
            for m in range(j + 1, BLOCK):
                cols[m] = cols[m] - ratio * jnp.broadcast_to(cols[j][m : m + 1, :], (BLOCK, HALF))
            for h in range(2):
                wide[h] = wide[h] - ratio * jnp.broadcast_to(wide[h][j : j + 1, :], (BLOCK, HALF))
            diag = diag - ratio * jnp.broadcast_to(diag[j : j + 1, :], (BLOCK, HALF))
        scale = lax.rsqrt(scale)
        done = jnp.concatenate([wide[0] * scale, wide[1] * scale], axis=1)
        inverse_ref[at : at + BLOCK, :] = jnp.where(lane < at + BLOCK, done, 0.0)
        upper_ref[at : at + BLOCK, :] = jnp.where(lane >= at + BLOCK, done, 0.0)
        upper_ref[at : at + BLOCK, base : base + HALF] = jnp.where(
            inside & (lane_half - off >= sub), diag * scale, upper_ref[at : at + BLOCK, base : base + HALF]
        )
        if at + BLOCK < PANEL:
            a, b, c = thirds(done)
            right = jnp.concatenate([a, b, a, c, a, b], axis=0)
            left = jnp.concatenate([a, a, b, a, c, b], axis=0)
            prod = lax.dot_general(left.T[at + BLOCK :, :], right, (((1,), (0,)), ((), ())), preferred_element_type=jnp.float32)
            rest = work[at + BLOCK :, :]
            lanes = lax.broadcasted_iota(jnp.int32, rest.shape, 1)
            rest = jnp.where((lanes >= at) & (lanes < at + BLOCK), 0.0, rest)
            work[at + BLOCK :, :] = rest - prod


WIDTH = 1024
STEP = 512
F32 = jnp.float32
BF16 = jnp.bfloat16
EARLY_ROWS = 9216
FIRST_ROWS = 1024
LAST_ROWS = 3072


def dot(left, right):
    return jnp.dot(left, right, preferred_element_type=F32)


def exact(left, right):
    return jnp.dot(left, right, precision=lax.Precision.HIGHEST, preferred_element_type=F32)


def pairs():
    return [(i, j) for i in range(4) for j in range(i, 4)]


def add_slabs(ref, at, value):
    rows = value.shape[0]
    for n in range(value.shape[1] // HALF):
        ref[at + n * rows : at + (n + 1) * rows, :] += value[:, n * HALF : (n + 1) * HALF]


def read_slabs(ref, at, rows, columns):
    return jnp.concatenate([ref[at + n * rows : at + (n + 1) * rows, :] for n in range(columns // HALF)], axis=1)


def products_kernel(earlier_ref, panels_ref, out_ref):
    @pl.when(pl.program_id(0) == 0)
    def _():
        out_ref[...] = jnp.zeros_like(out_ref)

    order = pairs()
    for i in range(4):
        turned = earlier_ref[:, i * PANEL : (i + 1) * PANEL].T
        value = dot(turned, panels_ref[...])
        for n in range(4):
            at = n * WIDTH + i * PANEL
            out_ref[at : at + PANEL, :] += value[:, n * HALF : (n + 1) * HALF]
        for j in range(i, 4):
            add_slabs(out_ref, 4 * WIDTH + order.index((i, j)) * 512, dot(turned, earlier_ref[:, j * PANEL : (j + 1) * PANEL]))


def add_gram(top, low, others, out_ref, mixed, at):
    top_t, low_t = top.T, low.T
    add_slabs(out_ref, at, dot(top_t, top) + dot(low_t, low))
    mixed[...] += dot(top_t, low)
    add_slabs(out_ref, at + 512, dot(top_t, others) + dot(low_t, others))


def close_gram(out_ref, mixed, at):
    value = mixed[...]
    add_slabs(out_ref, at, value + value.T)


def first_kernel(
    total, sums_ref, earlier_ref, panels_ref,
    top_ref, low_ref, flat_ref, early_ref, second_ref, left_ref, meet_ref, out_ref,
    coeffs, near, off_top, off_low, mixed,
):
    step = pl.program_id(0)

    @pl.when(step == 0)
    def _():
        scale = 1.0 / total
        for n, (i, j) in enumerate(pairs()):
            block = read_slabs(sums_ref, 4 * WIDTH + n * 512, PANEL, PANEL) * scale
            if i == j:
                rows = lax.broadcasted_iota(jnp.int32, block.shape, 0)
                columns = lax.broadcasted_iota(jnp.int32, block.shape, 1)
                block = block - (rows == columns).astype(F32)
            for r, c, value in [(i, j, block)] + ([(j, i, block.T)] if i != j else []):
                top, low = halves(value)
                off_top[r * PANEL : (r + 1) * PANEL, c * PANEL : (c + 1) * PANEL] = top
                off_low[r * PANEL : (r + 1) * PANEL, c * PANEL : (c + 1) * PANEL] = low
        for n in range(4):
            coeffs[:, n * HALF : (n + 1) * HALF] = (sums_ref[n * WIDTH : (n + 1) * WIDTH, :] * scale).astype(BF16)
        early = coeffs[...]
        for i in range(4):
            at = slice(i * PANEL, (i + 1) * PANEL)
            own = jnp.concatenate([sums_ref[n * WIDTH + i * PANEL : n * WIDTH + (i + 1) * PANEL, :] for n in range(4)], axis=1) * scale
            value = own - early[at, :].astype(F32) - (dot(off_top[at, :], early) + dot(off_low[at, :], early))
            near[at, :] = value[:, :PANEL].astype(BF16)
            left_ref[at, :] = value[:, :PANEL] - value[:, :PANEL].astype(BF16).astype(F32)
            second_ref[at, :] = value[:, PANEL:]
        meet = jnp.zeros((PANEL, PANEL), F32)
        for i in range(4):
            at = slice(i * PANEL, (i + 1) * PANEL)
            value = left_ref[at, :] - (dot(off_top[at, :], near[...]) + dot(off_low[at, :], near[...]))
            left_ref[at, :] = value
            top, low = halves(value.T)
            meet = meet + dot(top, early[at, PANEL:]) + dot(low, early[at, PANEL:])
        meet_ref[...] = meet
        early_ref[...] = early[:, PANEL:]
        out_ref[...] = jnp.zeros_like(out_ref)
        mixed[...] = jnp.zeros_like(mixed)

    space = earlier_ref[...]
    flat = panels_ref[...].astype(F32) - dot(space, coeffs[...])
    flat_ref[...] = flat[:, PANEL:]
    once = flat[:, :PANEL].astype(BF16)
    twice = once.astype(F32) - dot(space, near[...])
    top, low = halves(twice)
    top_ref[...] = top
    low_ref[...] = low
    add_gram(top, low, panels_ref[:, PANEL:], out_ref, mixed, 0)

    @pl.when(step == pl.num_programs(0) - 1)
    def _():
        close_gram(out_ref, mixed, 0)


def normalized(top, low, turned_top, turned_low):
    return (dot(top, turned_top) + (dot(top, turned_low) + dot(low, turned_top))).astype(BF16)


def second_kernel(
    total, sums_ref, left_ref, second_ref, meet_ref, earlier_ref, top_ref, low_ref, flat_ref, later_ref,
    upper_ref, basis_ref, newtop_ref, newlow_ref, out_ref,
    work, inverse, turned_top, turned_low, fresh_b, near_e, near_q, mixed,
):
    step = pl.program_id(0)

    @pl.when(step == 0)
    def _():
        scale = 1.0 / total
        work[...] = read_slabs(sums_ref, 0, PANEL, PANEL) * scale
        factor(work, upper_ref, inverse)
        turn = inverse[...].T
        turned_top[...], turned_low[...] = halves(turn)
        fresh = exact(inverse[...], read_slabs(sums_ref, 512, PANEL, PANEL) * scale)
        fresh_b[...] = fresh.astype(BF16)
        rounded = fresh.astype(BF16).astype(F32)
        near_q[...] = (fresh - rounded - exact(inverse[...], meet_ref[...])).astype(BF16)
        back = exact(turn, rounded)
        near_e[...] = (second_ref[...] - exact(left_ref[...], back)).astype(BF16)
        out_ref[...] = jnp.zeros_like(out_ref)
        mixed[...] = jnp.zeros_like(mixed)

    newcols = normalized(top_ref[...], low_ref[...], turned_top[...], turned_low[...])
    basis_ref[...] = newcols
    once = (flat_ref[...] - dot(newcols, fresh_b[...])).astype(BF16)
    twice = once.astype(F32) - (dot(earlier_ref[...], near_e[...]) + dot(newcols, near_q[...]))
    top, low = halves(twice)
    newtop_ref[...] = top
    newlow_ref[...] = low
    add_gram(top, low, later_ref[...], out_ref, mixed, 0)
    add_slabs(out_ref, 1536, dot(newcols.T, later_ref[...]))

    @pl.when(step == pl.num_programs(0) - 1)
    def _():
        close_gram(out_ref, mixed, 0)


def third_kernel(
    total, sums_ref, first_upper_ref, top_ref, low_ref, _, factors_ref, shift_ref, basis_ref,
    work, inverse, turned_top, turned_low,
):
    @pl.when(pl.program_id(0) == 0)
    def _():
        scale = 1.0 / total
        work[...] = read_slabs(sums_ref, 0, PANEL, PANEL) * scale
        factors_ref[0] = first_upper_ref[...]
        factor(work, factors_ref.at[1], inverse)
        turned_top[...], turned_low[...] = halves(inverse[...].T)
        shift_ref[:PANEL, :] = read_slabs(sums_ref, 1536, PANEL, 512) * scale
        shift_ref[PANEL:, :] = exact(inverse[...], read_slabs(sums_ref, 512, PANEL, 512) * scale)

    basis_ref[...] = normalized(top_ref[...], low_ref[...], turned_top[...], turned_low[...])


def whole(*shape):
    return pl.BlockSpec(shape, lambda n: (0,) * len(shape))


def rows(columns, place=0, step=STEP):
    return pl.BlockSpec((step, columns), lambda n: (n, place))


def shape(*lengths, dtype=F32):
    return jax.ShapeDtypeStruct(lengths, dtype)


def call(kernel, steps, name, **options):
    return pl.pallas_call(
        kernel,
        grid=(steps,),
        compiler_params=pltpu.CompilerParams(dimension_semantics=("arbitrary",), vmem_limit_bytes=56 * 2**20),
        name=name,
        **options,
    )


def body(earlier, snapshots, later):
    local = earlier.shape[0]
    total = local * lax.axis_size(AXES)
    steps = local // STEP
    square = pltpu.VMEM((PANEL, PANEL), F32)
    small = pltpu.VMEM((PANEL, PANEL), BF16)

    partial = call(
        products_kernel, local // 1024, "products",
        in_specs=[rows(WIDTH, step=1024), rows(512, step=1024)],
        out_specs=whole(EARLY_ROWS, HALF),
        out_shape=shape(EARLY_ROWS, HALF),
    )(earlier, snapshots)
    early_sums = summed(partial, colored(EARLY_ROWS, THREE), 1)
    top, low, flat, early, second, left, meet, partial = call(
        functools.partial(first_kernel, total), steps, "first",
        in_specs=[whole(EARLY_ROWS, HALF), rows(WIDTH), rows(512)],
        out_specs=[rows(PANEL), rows(PANEL), rows(PANEL), whole(WIDTH, PANEL), whole(WIDTH, PANEL), whole(WIDTH, PANEL),
                   whole(PANEL, PANEL), whole(FIRST_ROWS, HALF)],
        out_shape=[shape(local, PANEL, dtype=BF16), shape(local, PANEL, dtype=BF16), shape(local, PANEL),
                   shape(WIDTH, PANEL, dtype=BF16), shape(WIDTH, PANEL), shape(WIDTH, PANEL), shape(PANEL, PANEL),
                   shape(FIRST_ROWS, HALF)],
        scratch_shapes=[pltpu.VMEM((WIDTH, 512), BF16), pltpu.VMEM((WIDTH, PANEL), BF16), pltpu.VMEM((WIDTH, WIDTH), BF16),
                        pltpu.VMEM((WIDTH, WIDTH), BF16), square],
    )(early_sums, earlier, snapshots)
    first_sums = summed(partial, colored(FIRST_ROWS, ONE), 2)
    upper, basis, newtop, newlow, partial = call(
        functools.partial(second_kernel, total), steps, "second",
        in_specs=[whole(FIRST_ROWS, HALF), whole(WIDTH, PANEL), whole(WIDTH, PANEL), whole(PANEL, PANEL), rows(WIDTH),
                  rows(PANEL), rows(PANEL), rows(PANEL), rows(512)],
        out_specs=[whole(PANEL, PANEL), rows(PANEL), rows(PANEL), rows(PANEL), whole(LAST_ROWS, HALF)],
        out_shape=[shape(PANEL, PANEL), shape(local, 512, dtype=BF16), shape(local, PANEL, dtype=BF16),
                   shape(local, PANEL, dtype=BF16), shape(LAST_ROWS, HALF)],
        scratch_shapes=[square, square, small, small, small, pltpu.VMEM((WIDTH, PANEL), BF16), small, square],
    )(first_sums, left, second, meet, earlier, top, low, flat, later)
    last_sums = summed(partial, colored(LAST_ROWS, ONE), 3)
    factors, shift_block, basis = call(
        functools.partial(third_kernel, total), steps, "third",
        in_specs=[whole(LAST_ROWS, HALF), whole(PANEL, PANEL), rows(PANEL), rows(PANEL), pl.BlockSpec(memory_space=pl.ANY)],
        out_specs=[whole(2, PANEL, PANEL), whole(512, 512), rows(PANEL, 1)],
        out_shape=[shape(2, PANEL, PANEL), shape(512, 512), shape(local, 512, dtype=BF16)],
        scratch_shapes=[square, square, small, small],
        input_output_aliases={4: 2},
    )(last_sums, upper, newtop, newlow, basis)
    return (basis, factors, shift_block)


def solution(mesh):
    torus = Mesh(mesh.devices.reshape(4, 4, 4, mesh.shape["grp"]), AXES)
    spec = P(AXES, None)
    return jax.shard_map(
        body, mesh=torus, in_specs=(spec, spec, spec), out_specs=(spec, P(), P()), check_vma=False
    )
```

```python
import functools
import itertools

import jax
import jax.numpy as jnp
from jax import lax
from jax.experimental import pallas as pl
from jax.experimental.pallas import tpu as pltpu
from jax.sharding import Mesh
from jax.sharding import PartitionSpec as P

PANEL = 256
BLOCK = 32
HALF = 128
F32 = jnp.float32
BF16 = jnp.bfloat16
MESH = pl.DeviceIdType.MESH
AXES = ("rows_0", "rows_1", "rows_2", "grp")


def thirds(value):
    top = value.astype(jnp.bfloat16)
    rest = value - top.astype(jnp.float32)
    middle = rest.astype(jnp.bfloat16)
    low = (rest - middle.astype(jnp.float32)).astype(jnp.bfloat16)
    return top, middle, low


def halves(value):
    top = value.astype(jnp.bfloat16)
    return top, (value - top.astype(jnp.float32)).astype(jnp.bfloat16)


def length_of(axis):
    return 2 if axis == "grp" or ":" in axis else 4


def size_of(stage):
    size = 1
    for axis in stage:
        size *= length_of(axis)
    return size


def offsets(stage):
    return [o for o in itertools.product(*[range(length_of(axis)) for axis in stage]) if any(o)]


def moved(axis, shift):
    name, _, pairing = axis.partition(":")
    at = lax.axis_index(name)
    if pairing == "a":
        return name, at + 1 - 2 * lax.rem(at, 2)
    if pairing == "b":
        return name, lax.rem(at + 3 + 2 * lax.rem(at, 2), 4)
    return name, lax.rem(at + shift, length_of(axis))


def part_of(axis, at):
    pairing = axis.partition(":")[2]
    if pairing == "a":
        return lax.rem((at + 1) // 2, 2)
    if pairing == "b":
        return at // 2
    return at


def peer_of(stage, offset):
    return dict(moved(axis, shift) for axis, shift in zip(stage, offset) if shift)


def place_in(stage, offset=None):
    place = 0
    for n, axis in enumerate(stage):
        at = moved(axis, offset[n])[1] if offset is not None and offset[n] else lax.axis_index(axis.partition(":")[0])
        place = place * length_of(axis) + part_of(axis, at)
    return place


def greet(stages):
    peers = []
    for stage in stages:
        for offset in offsets(stage):
            key = tuple((axis, shift) for axis, shift in zip(stage, offset) if shift)
            if key not in peers:
                peers.append(key)
    barrier = pltpu.get_barrier_semaphore()
    for key in peers:
        pl.semaphore_signal(
            barrier, inc=1, device_id=peer_of([a for a, _ in key], [n for _, n in key]), device_id_type=MESH
        )
    return lambda: pl.semaphore_wait(barrier, len(peers))


def levels_of(rows, stages):
    for stage in stages:
        rows //= size_of(stage)
        assert rows % 8 == 0
        yield stage, offsets(stage), rows


def stream_scratch(streams):
    shapes = []
    for _, rows, stages in streams:
        for stage, offs, length in levels_of(rows, stages):
            shapes += [pltpu.VMEM((len(offs), length, HALF), F32), pltpu.VMEM((length, HALF), F32)]
            shapes += [pltpu.SemaphoreType.DMA((len(offs),))] * 4
    return shapes


def copy_to(src, dst, send, recv, stage, offset):
    return pltpu.make_async_remote_copy(
        src_ref=src, dst_ref=dst, send_sem=send, recv_sem=recv, device_id=peer_of(stage, offset), device_id_type=MESH
    )


def stream(x_ref, o_ref, start, rows, stages, scratch, sent):
    levels = [level + tuple(next(scratch) for _ in range(6)) for level in levels_of(rows, stages)]
    where, src, base = start, x_ref, start
    for n, (stage, offs, length, slots, acc, send, recv, _, _) in enumerate(levels):
        copies = []
        for k, offset in enumerate(offs):
            at = pl.multiple_of(base + place_in(stage, offset) * length, 8)
            copies.append(copy_to(src.at[pl.ds(at, length), :], slots.at[k], send.at[k], recv.at[k], stage, offset))
            copies[-1].start()
        sent += copies
        yield
        own = place_in(stage) * length
        for copy in copies:
            copy.wait_recv()
        value = src[pl.ds(pl.multiple_of(base + own, 8), length), :]
        for k in range(len(offs)):
            value = value + slots[k]
        where = where + own
        if n + 1 < len(levels):
            acc[...] = value
        else:
            o_ref[pl.ds(pl.multiple_of(where, 8), length), :] = value
        src, base = acc, 0
    for stage, offs, length, _, _, _, _, send, recv in reversed(levels):
        piece = o_ref.at[pl.ds(pl.multiple_of(where, 8), length), :]
        copies = [copy_to(piece, piece, send.at[k], recv.at[k], stage, offset) for k, offset in enumerate(offs)]
        for copy in copies:
            copy.start()
        sent += copies
        yield
        for copy in copies:
            copy.wait_recv()
        where = where - place_in(stage) * length


def advance(streams):
    for one in streams:
        next(one, None)


G, X, Y, Z = "grp", "rows_2", "rows_1", "rows_0"
ORDERS = [((G,), (X,), (Y,), (Z,)), ((G,), (Y,), (Z,), (X,)), ((G,), (Z,), (X,), (Y,))]
PLANES = [((G,), (X,), (Y, Z)), ((G,), (Y,), (Z, X)), ((G,), (Z,), (X, Y))]
AT_ONCE = [((G,), (X, Y, Z))]


def colored(rows, orders, count):
    return [(n * rows // count, rows // count, orders[n % len(orders)]) for n in range(count)]


def sum_kernel(streams, x_ref, o_ref, *scratch):
    ready = greet([stage for _, _, stages in streams for stage in stages])
    ready()
    scratch, sent = iter(scratch), []
    running = [stream(x_ref, o_ref, *one, scratch, sent) for one in streams]
    for _ in range(2 * max(len(stages) for _, _, stages in streams) + 1):
        advance(running)
    for copy in sent:
        copy.wait_send()


def summed(x, streams, cid):
    return pl.pallas_call(
        functools.partial(sum_kernel, streams),
        out_shape=jax.ShapeDtypeStruct(x.shape, x.dtype),
        in_specs=[pl.BlockSpec(memory_space=pltpu.VMEM)],
        out_specs=pl.BlockSpec(memory_space=pltpu.VMEM),
        scratch_shapes=stream_scratch(streams),
        compiler_params=pltpu.CompilerParams(collective_id=cid, has_side_effects=True, vmem_limit_bytes=24 * 2**20),
        name="summed%d" % cid,
    )(x)


def factor(work, upper_ref, inverse_ref):
    lane = lax.broadcasted_iota(jnp.int32, (BLOCK, PANEL), 1)
    sub = lax.broadcasted_iota(jnp.int32, (BLOCK, HALF), 0)
    lane_half = lax.broadcasted_iota(jnp.int32, (BLOCK, HALF), 1)
    for k in range(PANEL // BLOCK):
        at = k * BLOCK
        rows = work[at : at + BLOCK, :]
        base = at // HALF * HALF
        off = at - base
        diag = rows[:, base : base + HALF]
        cols = [jnp.broadcast_to(diag[:, off + j : off + j + 1], (BLOCK, HALF)) for j in range(BLOCK)]
        eye = (lane_half == sub + off).astype(jnp.float32)
        wide = [rows[:, :HALF], rows[:, HALF:]]
        own = base // HALF
        inside = (lane_half >= off) & (lane_half < off + BLOCK)
        wide[own] = jnp.where(inside, eye, wide[own])
        scale = jnp.zeros((BLOCK, HALF), jnp.float32)
        for j in range(BLOCK):
            pivot = jnp.broadcast_to(cols[j][j : j + 1, :], (BLOCK, HALF))
            scale = jnp.where(sub == j, pivot, scale)
            if j == BLOCK - 1:
                break
            ratio = cols[j] * (1.0 / pivot)
            ratio = jnp.where(sub > j, ratio, 0.0)
            for m in range(j + 1, BLOCK):
                cols[m] = cols[m] - ratio * jnp.broadcast_to(cols[j][m : m + 1, :], (BLOCK, HALF))
            for h in range(2):
                wide[h] = wide[h] - ratio * jnp.broadcast_to(wide[h][j : j + 1, :], (BLOCK, HALF))
            diag = diag - ratio * jnp.broadcast_to(diag[j : j + 1, :], (BLOCK, HALF))
        scale = lax.rsqrt(scale)
        done = jnp.concatenate([wide[0] * scale, wide[1] * scale], axis=1)
        inverse_ref[at : at + BLOCK, :] = jnp.where(lane < at + BLOCK, done, 0.0)
        upper_ref[at : at + BLOCK, :] = jnp.where(lane >= at + BLOCK, done, 0.0)
        upper_ref[at : at + BLOCK, base : base + HALF] = jnp.where(
            inside & (lane_half - off >= sub), diag * scale, upper_ref[at : at + BLOCK, base : base + HALF]
        )
        if at + BLOCK < PANEL:
            a, b, c = thirds(done)
            right = jnp.concatenate([a, b, a, c, a, b], axis=0)
            left = jnp.concatenate([a, a, b, a, c, b], axis=0)
            prod = lax.dot_general(left.T[at + BLOCK :, :], right, (((1,), (0,)), ((), ())), preferred_element_type=jnp.float32)
            rest = work[at + BLOCK :, :]
            lanes = lax.broadcasted_iota(jnp.int32, rest.shape, 1)
            rest = jnp.where((lanes >= at) & (lanes < at + BLOCK), 0.0, rest)
            work[at + BLOCK :, :] = rest - prod


WIDTH = 1024
STEP = 1024
EARLY_ROWS = 9216
FIRST_ROWS = 1024
LAST_ROWS = 3072


def dot(left, right):
    return jnp.dot(left, right, preferred_element_type=F32)


def exact(left, right):
    return jnp.dot(left, right, precision=lax.Precision.HIGHEST, preferred_element_type=F32)


PAIRS = [(i, j) for i in range(4) for j in range(i, 4)]


def span(n, length=PANEL):
    return slice(n * length, (n + 1) * length)


def put_slabs(ref, at, value):
    rows = value.shape[0]
    for n in range(value.shape[1] // HALF):
        ref[at + n * rows : at + (n + 1) * rows, :] = value[:, span(n, HALF)]


def add_slabs(ref, at, value):
    rows = value.shape[0]
    for n in range(value.shape[1] // HALF):
        ref[at + n * rows : at + (n + 1) * rows, :] += value[:, span(n, HALF)]


def read_slabs(ref, at, rows, columns):
    return jnp.concatenate([ref[at + n * rows : at + (n + 1) * rows, :] for n in range(columns // HALF)], axis=1)


def add_gram(top, low, others, out_ref, mixed):
    top_t, low_t = top.T, low.T
    add_slabs(out_ref, 0, dot(top_t, top) + dot(low_t, low))
    mixed[...] += dot(top_t, low)
    add_slabs(out_ref, 512, dot(top_t, others) + dot(low_t, others))


def close_gram(out_ref, mixed):
    value = mixed[...]
    add_slabs(out_ref, 0, value + value.T)


EARLY_STREAMS = colored(EARLY_ROWS, ORDERS, 9)


def first_kernel(
    total, earlier_hbm, panels_hbm,
    top_hbm, low_hbm, flat_hbm, second_ref, left_ref, meet_ref, out_ref,
    earlier, panels, turned, partial, sums, off, coeffs, near, mixed, top_all, low_all, flat_all, load, save, *scratch,
):
    ready = greet(ORDERS[0])
    scale = 1.0 / total
    chunks = earlier.shape[0] // 512
    loads = []
    for n in range(chunks):
        at = pl.ds(n * 512, 512)
        loads.append((
            pltpu.make_async_copy(earlier_hbm.at[at, :], earlier.at[at, :], load.at[0, n]),
            pltpu.make_async_copy(panels_hbm.at[at, :], panels.at[at, :], load.at[1, n]),
        ))
        for copy in loads[-1]:
            copy.start()
    for n in range(chunks):
        loads[n][0].wait()
        for i in range(4):
            turned[span(i), span(n, 512)] = earlier[span(n, 512), span(i)].T
    for n in range(chunks):
        loads[n][1].wait()
    for i in range(4):
        value = dot(turned[span(i), :], panels[...])
        for n in range(4):
            partial[n * WIDTH + i * PANEL : n * WIDTH + (i + 1) * PANEL, :] = value[:, span(n, HALF)]

    scratch, sent = iter(scratch), []
    running = [stream(partial, sums, *one, scratch, sent) for one in EARLY_STREAMS]
    lead, rest = running[:4], running[4:]

    def gram_row(i):
        for j in range(i, 4):
            put_slabs(partial, 4 * WIDTH + PAIRS.index((i, j)) * 512, dot(turned[span(i), :], earlier[:, span(j)]))

    ready()
    advance(lead)
    gram_row(0)
    advance(lead)
    for i in range(1, 4):
        gram_row(i)
    advance(rest)
    for _ in range(7):
        advance(lead)
        advance(rest)

    for n in range(4):
        value = (sums[span(n, WIDTH), :] * scale).astype(BF16)
        coeffs[:WIDTH, span(n, HALF)] = value
        coeffs[WIDTH:, span(n, HALF)] = value
    saves = []
    for n in range(earlier.shape[0] // STEP):
        at = span(n, STEP)
        flat = panels[at, :].astype(F32) - dot(earlier[at, :], coeffs[:WIDTH, :])
        top_all[at, :] = flat[:, :PANEL].astype(BF16)
        flat_all[at, :] = flat[:, PANEL:]
        saves.append(pltpu.make_async_copy(flat_all.at[at, :], flat_hbm.at[at, :], save.at[0, n]))
        saves[-1].start()
    advance(rest)

    for n, (i, j) in enumerate(PAIRS):
        block = read_slabs(sums, 4 * WIDTH + n * 512, PANEL, PANEL) * scale
        if i == j:
            rows = lax.broadcasted_iota(jnp.int32, block.shape, 0)
            columns = lax.broadcasted_iota(jnp.int32, block.shape, 1)
            block = block - (rows == columns).astype(F32)
        for k, value in enumerate(halves(block)):
            off[span(i), k * WIDTH + j * PANEL : k * WIDTH + (j + 1) * PANEL] = value
            if i != j:
                off[span(j), k * WIDTH + i * PANEL : k * WIDTH + (i + 1) * PANEL] = value.T
    beyond = dot(off[...], coeffs[...])
    for n in range(4):
        value = sums[span(n, WIDTH), :] * scale
        value = value - coeffs[:WIDTH, span(n, HALF)].astype(F32) - beyond[:, span(n, HALF)]
        if n < 2:
            near[:WIDTH, span(n, HALF)] = value.astype(BF16)
            near[WIDTH:, span(n, HALF)] = value.astype(BF16)
            left_ref[:, span(n, HALF)] = value - value.astype(BF16).astype(F32)
        else:
            second_ref[:, span(n - 2, HALF)] = value

    out_ref[...] = jnp.zeros_like(out_ref)
    mixed[...] = jnp.zeros_like(mixed)
    for n in range(earlier.shape[0] // STEP):
        at = span(n, STEP)
        twice = top_all[at, :].astype(F32) - dot(earlier[at, :], near[:WIDTH, :])
        top, low = halves(twice)
        top_all[at, :] = top
        low_all[at, :] = low
        saves.append(pltpu.make_async_copy(top_all.at[at, :], top_hbm.at[at, :], save.at[1, n]))
        saves[-1].start()
        saves.append(pltpu.make_async_copy(low_all.at[at, :], low_hbm.at[at, :], save.at[2, n]))
        saves[-1].start()
        add_gram(top, low, panels[at, PANEL:], out_ref, mixed)
    close_gram(out_ref, mixed)
    left = left_ref[...] - dot(off[...], near[...])
    left_ref[...] = left
    left_t = left.T
    top, low = halves(left_t)
    meet_ref[...] = dot(top, coeffs[:WIDTH, PANEL:]) + dot(low, coeffs[:WIDTH, PANEL:])
    for copy in saves:
        copy.wait()
    for copy in sent:
        copy.wait_send()


def normalized(top, low, turned_top, turned_low):
    return (dot(top, turned_top) + (dot(top, turned_low) + dot(low, turned_top))).astype(BF16)


def second_kernel(
    total, sums_ref, left_ref, second_ref, meet_ref, earlier_ref, top_ref, low_ref, flat_ref, later_ref,
    upper_ref, basis_ref, newtop_ref, newlow_ref, out_ref,
    work, inverse, turned_top, turned_low, fresh_b, near_e, near_q, mixed,
):
    step = pl.program_id(0)

    @pl.when(step == 0)
    def _():
        scale = 1.0 / total
        work[...] = read_slabs(sums_ref, 0, PANEL, PANEL) * scale
        factor(work, upper_ref, inverse)
        turn = inverse[...].T
        turned_top[...], turned_low[...] = halves(turn)
        fresh = exact(inverse[...], read_slabs(sums_ref, 512, PANEL, PANEL) * scale)
        fresh_b[...] = fresh.astype(BF16)
        rounded = fresh.astype(BF16).astype(F32)
        near_q[...] = (fresh - rounded - exact(inverse[...], meet_ref[...])).astype(BF16)
        back = exact(turn, rounded)
        near_e[...] = (second_ref[...] - exact(left_ref[...], back)).astype(BF16)
        out_ref[...] = jnp.zeros_like(out_ref)
        mixed[...] = jnp.zeros_like(mixed)

    newcols = normalized(top_ref[...], low_ref[...], turned_top[...], turned_low[...])
    basis_ref[...] = newcols
    once = (flat_ref[...] - dot(newcols, fresh_b[...])).astype(BF16)
    twice = once.astype(F32) - (dot(earlier_ref[...], near_e[...]) + dot(newcols, near_q[...]))
    top, low = halves(twice)
    newtop_ref[...] = top
    newlow_ref[...] = low
    add_gram(top, low, later_ref[...], out_ref, mixed)
    add_slabs(out_ref, 1536, dot(newcols.T, later_ref[...]))

    @pl.when(step == pl.num_programs(0) - 1)
    def _():
        close_gram(out_ref, mixed)


def third_kernel(
    total, sums_ref, first_upper_ref, top_ref, low_ref, _, factors_ref, shift_ref, basis_ref,
    work, inverse, turned_top, turned_low,
):
    @pl.when(pl.program_id(0) == 0)
    def _():
        scale = 1.0 / total
        work[...] = read_slabs(sums_ref, 0, PANEL, PANEL) * scale
        factors_ref[0] = first_upper_ref[...]
        factor(work, factors_ref.at[1], inverse)
        turned_top[...], turned_low[...] = halves(inverse[...].T)
        shift_ref[:PANEL, :] = read_slabs(sums_ref, 1536, PANEL, 512) * scale
        shift_ref[PANEL:, :] = exact(inverse[...], read_slabs(sums_ref, 512, PANEL, 512) * scale)

    basis_ref[...] = normalized(top_ref[...], low_ref[...], turned_top[...], turned_low[...])


def whole(*shape):
    return pl.BlockSpec(shape, lambda n: (0,) * len(shape))


def rows(columns, place=0, step=STEP):
    return pl.BlockSpec((step, columns), lambda n: (n, place))


def shape(*lengths, dtype=F32):
    return jax.ShapeDtypeStruct(lengths, dtype)


def call(kernel, steps, name, **options):
    return pl.pallas_call(
        kernel,
        grid=(steps,),
        compiler_params=pltpu.CompilerParams(dimension_semantics=("arbitrary",), vmem_limit_bytes=40 * 2**20),
        name=name,
        **options,
    )


def body(earlier, snapshots, later):
    local = earlier.shape[0]
    total = local * lax.axis_size(AXES)
    steps = local // STEP
    square = pltpu.VMEM((PANEL, PANEL), F32)
    small = pltpu.VMEM((PANEL, PANEL), BF16)
    inside, outside = pl.BlockSpec(memory_space=pltpu.VMEM), pl.BlockSpec(memory_space=pl.ANY)

    top, low, flat, second, left, meet, partial = pl.pallas_call(
        functools.partial(first_kernel, total),
        in_specs=[outside] * 2,
        out_specs=[outside] * 3 + [inside] * 4,
        out_shape=[shape(local, PANEL, dtype=BF16), shape(local, PANEL, dtype=BF16), shape(local, PANEL),
                   shape(WIDTH, PANEL), shape(WIDTH, PANEL), shape(PANEL, PANEL), shape(FIRST_ROWS, HALF)],
        scratch_shapes=[pltpu.VMEM((local, WIDTH), BF16), pltpu.VMEM((local, 512), BF16), pltpu.VMEM((WIDTH, local), BF16),
                        pltpu.VMEM((EARLY_ROWS, HALF), F32), pltpu.VMEM((EARLY_ROWS, HALF), F32),
                        pltpu.VMEM((WIDTH, 2 * WIDTH), BF16), pltpu.VMEM((2 * WIDTH, 512), BF16),
                        pltpu.VMEM((2 * WIDTH, PANEL), BF16), square,
                        pltpu.VMEM((local, PANEL), BF16), pltpu.VMEM((local, PANEL), BF16), pltpu.VMEM((local, PANEL), F32),
                        pltpu.SemaphoreType.DMA((2, local // 512)), pltpu.SemaphoreType.DMA((3, steps))]
        + stream_scratch(EARLY_STREAMS),
        compiler_params=pltpu.CompilerParams(collective_id=1, has_side_effects=True, vmem_limit_bytes=62 * 2**20),
        name="first",
    )(earlier, snapshots)
    first_sums = summed(partial, colored(FIRST_ROWS, AT_ONCE, 1), 2)
    upper, basis, newtop, newlow, partial = call(
        functools.partial(second_kernel, total), steps, "second",
        in_specs=[whole(FIRST_ROWS, HALF), whole(WIDTH, PANEL), whole(WIDTH, PANEL), whole(PANEL, PANEL), rows(WIDTH),
                  rows(PANEL), rows(PANEL), rows(PANEL), rows(512)],
        out_specs=[whole(PANEL, PANEL), rows(PANEL), rows(PANEL), rows(PANEL), whole(LAST_ROWS, HALF)],
        out_shape=[shape(PANEL, PANEL), shape(local, 512, dtype=BF16), shape(local, PANEL, dtype=BF16),
                   shape(local, PANEL, dtype=BF16), shape(LAST_ROWS, HALF)],
        scratch_shapes=[square, square, small, small, small, pltpu.VMEM((WIDTH, PANEL), BF16), small, square],
    )(first_sums, left, second, meet, earlier, top, low, flat, later)
    last_sums = summed(partial, colored(LAST_ROWS, PLANES, 3), 3)
    factors, shift_block, basis = call(
        functools.partial(third_kernel, total), local // 2048, "third",
        in_specs=[whole(LAST_ROWS, HALF), whole(PANEL, PANEL), rows(PANEL, step=2048), rows(PANEL, step=2048), outside],
        out_specs=[whole(2, PANEL, PANEL), whole(512, 512), rows(PANEL, 1, step=2048)],
        out_shape=[shape(2, PANEL, PANEL), shape(512, 512), shape(local, 512, dtype=BF16)],
        scratch_shapes=[square, square, small, small],
        input_output_aliases={4: 2},
    )(last_sums, upper, newtop, newlow, basis)
    return (basis, factors, shift_block)


def solution(mesh):
    torus = Mesh(mesh.devices.reshape(4, 4, 4, mesh.shape["grp"]), AXES)
    spec = P(AXES, None)
    return jax.shard_map(
        body, mesh=torus, in_specs=(spec, spec, spec), out_specs=(spec, P(), P()), check_vma=False
    )
```

```python
import functools
import itertools

import jax
import jax.numpy as jnp
from jax import lax
from jax.experimental import pallas as pl
from jax.experimental.pallas import tpu as pltpu
from jax.sharding import Mesh
from jax.sharding import PartitionSpec as P

PANEL = 256
BLOCK = 32
HALF = 128
F32 = jnp.float32
BF16 = jnp.bfloat16
MESH = pl.DeviceIdType.MESH
AXES = ("rows_0", "rows_1", "rows_2", "grp")


def thirds(value):
    top = value.astype(jnp.bfloat16)
    rest = value - top.astype(jnp.float32)
    middle = rest.astype(jnp.bfloat16)
    low = (rest - middle.astype(jnp.float32)).astype(jnp.bfloat16)
    return top, middle, low


def halves(value):
    top = value.astype(jnp.bfloat16)
    return top, (value - top.astype(jnp.float32)).astype(jnp.bfloat16)


def length_of(axis):
    return 2 if axis == "grp" or ":" in axis else 4


def size_of(stage):
    size = 1
    for axis in stage:
        size *= length_of(axis)
    return size


def offsets(stage):
    return [o for o in itertools.product(*[range(length_of(axis)) for axis in stage]) if any(o)]


def moved(axis, shift):
    name, _, pairing = axis.partition(":")
    at = lax.axis_index(name)
    if pairing == "a":
        return name, at + 1 - 2 * lax.rem(at, 2)
    if pairing == "b":
        return name, lax.rem(at + 3 + 2 * lax.rem(at, 2), 4)
    return name, lax.rem(at + shift, length_of(axis))


def part_of(axis, at):
    pairing = axis.partition(":")[2]
    if pairing == "a":
        return lax.rem((at + 1) // 2, 2)
    if pairing == "b":
        return at // 2
    return at


def peer_of(stage, offset):
    return dict(moved(axis, shift) for axis, shift in zip(stage, offset) if shift)


def place_in(stage, offset=None):
    place = 0
    for n, axis in enumerate(stage):
        at = moved(axis, offset[n])[1] if offset is not None and offset[n] else lax.axis_index(axis.partition(":")[0])
        place = place * length_of(axis) + part_of(axis, at)
    return place


def greet(stages):
    peers = []
    for stage in stages:
        for offset in offsets(stage):
            key = tuple(sorted((axis, shift) for axis, shift in zip(stage, offset) if shift))
            if key not in peers:
                peers.append(key)
    barrier = pltpu.get_barrier_semaphore()
    for key in peers:
        pl.semaphore_signal(
            barrier, inc=1, device_id=peer_of([a for a, _ in key], [n for _, n in key]), device_id_type=MESH
        )
    return lambda: pl.semaphore_wait(barrier, len(peers))


def levels_of(rows, stages):
    for stage in stages:
        rows //= size_of(stage)
        assert rows % 8 == 0
        yield stage, offsets(stage), rows


def stream_scratch(streams):
    shapes = []
    for _, rows, stages in streams:
        for stage, offs, length in levels_of(rows, stages):
            shapes += [pltpu.VMEM((len(offs), length, HALF), F32), pltpu.VMEM((length, HALF), F32)]
            shapes += [pltpu.SemaphoreType.DMA((len(offs),))] * 4
    return shapes


def copy_to(src, dst, send, recv, stage, offset):
    return pltpu.make_async_remote_copy(
        src_ref=src, dst_ref=dst, send_sem=send, recv_sem=recv, device_id=peer_of(stage, offset), device_id_type=MESH
    )


def stream(x_ref, o_ref, start, rows, stages, scratch, sent):
    levels = [level + tuple(next(scratch) for _ in range(6)) for level in levels_of(rows, stages)]
    where, src, base = start, x_ref, start
    for n, (stage, offs, length, slots, acc, send, recv, _, _) in enumerate(levels):
        copies = []
        for k, offset in enumerate(offs):
            at = pl.multiple_of(base + place_in(stage, offset) * length, 8)
            copies.append(copy_to(src.at[pl.ds(at, length), :], slots.at[k], send.at[k], recv.at[k], stage, offset))
            copies[-1].start()
        sent += copies
        yield
        own = place_in(stage) * length
        for copy in copies:
            copy.wait_recv()
        value = src[pl.ds(pl.multiple_of(base + own, 8), length), :]
        for k in range(len(offs)):
            value = value + slots[k]
        where = where + own
        if n + 1 < len(levels):
            acc[...] = value
        else:
            o_ref[pl.ds(pl.multiple_of(where, 8), length), :] = value
        src, base = acc, 0
    for stage, offs, length, _, _, _, _, send, recv in reversed(levels):
        piece = o_ref.at[pl.ds(pl.multiple_of(where, 8), length), :]
        copies = [copy_to(piece, piece, send.at[k], recv.at[k], stage, offset) for k, offset in enumerate(offs)]
        for copy in copies:
            copy.start()
        sent += copies
        yield
        for copy in copies:
            copy.wait_recv()
        where = where - place_in(stage) * length


def advance(streams):
    for one in streams:
        next(one, None)


G, X, Y, Z = "grp", "rows_2", "rows_1", "rows_0"
ORDERS = [((G,), (X,), (Y,), (Z,)), ((G,), (Y,), (Z,), (X,)), ((G,), (Z,), (X,), (Y,))]
PLANES = [((G,), (X,), (Y, Z)), ((G,), (Y,), (Z, X)), ((G,), (Z,), (X, Y))]
AT_ONCE = [((G,), (X, Y, Z))]


def colored(rows, orders, count):
    return [(n * rows // count, rows // count, orders[n % len(orders)]) for n in range(count)]


def factor(work, upper_ref, inverse_ref):
    lane = lax.broadcasted_iota(jnp.int32, (BLOCK, PANEL), 1)
    sub = lax.broadcasted_iota(jnp.int32, (BLOCK, HALF), 0)
    lane_half = lax.broadcasted_iota(jnp.int32, (BLOCK, HALF), 1)
    for k in range(PANEL // BLOCK):
        at = k * BLOCK
        rows = work[at : at + BLOCK, :]
        base = at // HALF * HALF
        off = at - base
        diag = rows[:, base : base + HALF]
        cols = [jnp.broadcast_to(diag[:, off + j : off + j + 1], (BLOCK, HALF)) for j in range(BLOCK)]
        eye = (lane_half == sub + off).astype(jnp.float32)
        wide = [rows[:, :HALF], rows[:, HALF:]]
        own = base // HALF
        inside = (lane_half >= off) & (lane_half < off + BLOCK)
        wide[own] = jnp.where(inside, eye, wide[own])
        scale = jnp.zeros((BLOCK, HALF), jnp.float32)
        for j in range(BLOCK):
            pivot = jnp.broadcast_to(cols[j][j : j + 1, :], (BLOCK, HALF))
            scale = jnp.where(sub == j, pivot, scale)
            if j == BLOCK - 1:
                break
            ratio = cols[j] * (1.0 / pivot)
            ratio = jnp.where(sub > j, ratio, 0.0)
            for m in range(j + 1, BLOCK):
                cols[m] = cols[m] - ratio * jnp.broadcast_to(cols[j][m : m + 1, :], (BLOCK, HALF))
            for h in range(2):
                wide[h] = wide[h] - ratio * jnp.broadcast_to(wide[h][j : j + 1, :], (BLOCK, HALF))
            diag = diag - ratio * jnp.broadcast_to(diag[j : j + 1, :], (BLOCK, HALF))
        scale = lax.rsqrt(scale)
        done = jnp.concatenate([wide[0] * scale, wide[1] * scale], axis=1)
        inverse_ref[at : at + BLOCK, :] = jnp.where(lane < at + BLOCK, done, 0.0)
        upper_ref[at : at + BLOCK, :] = jnp.where(lane >= at + BLOCK, done, 0.0)
        upper_ref[at : at + BLOCK, base : base + HALF] = jnp.where(
            inside & (lane_half - off >= sub), diag * scale, upper_ref[at : at + BLOCK, base : base + HALF]
        )
        if at + BLOCK < PANEL:
            a, b, c = thirds(done)
            right = jnp.concatenate([a, b, a, c, a, b], axis=0)
            left = jnp.concatenate([a, a, b, a, c, b], axis=0)
            prod = lax.dot_general(left.T[at + BLOCK :, :], right, (((1,), (0,)), ((), ())), preferred_element_type=jnp.float32)
            rest = work[at + BLOCK :, :]
            lanes = lax.broadcasted_iota(jnp.int32, rest.shape, 1)
            rest = jnp.where((lanes >= at) & (lanes < at + BLOCK), 0.0, rest)
            work[at + BLOCK :, :] = rest - prod
        yield


WIDTH = 1024
STEP = 1024
EARLY_ROWS = 9216
FIRST_ROWS = 1024
LAST_ROWS = 3072


def dot(left, right):
    return jnp.dot(left, right, preferred_element_type=F32)


def exact(left, right):
    return jnp.dot(left, right, precision=lax.Precision.HIGHEST, preferred_element_type=F32)


PAIRS = [(i, j) for j in range(4) for i in range(j + 1)]


def span(n, length=PANEL):
    return slice(n * length, (n + 1) * length)


def put_slabs(ref, at, value):
    rows = value.shape[0]
    for n in range(value.shape[1] // HALF):
        ref[at + n * rows : at + (n + 1) * rows, :] = value[:, span(n, HALF)]


def add_slabs(ref, at, value):
    rows = value.shape[0]
    for n in range(value.shape[1] // HALF):
        ref[at + n * rows : at + (n + 1) * rows, :] += value[:, span(n, HALF)]


def read_slabs(ref, at, rows, columns):
    return jnp.concatenate([ref[at + n * rows : at + (n + 1) * rows, :] for n in range(columns // HALF)], axis=1)


def add_gram(top, low, others, out_ref, mixed):
    top_t, low_t = top.T, low.T
    add_slabs(out_ref, 0, dot(top_t, top) + dot(low_t, low))
    mixed[...] += dot(top_t, low)
    if others is not None:
        add_slabs(out_ref, 512, dot(top_t, others) + dot(low_t, others))


def close_gram(out_ref, mixed):
    value = mixed[...]
    add_slabs(out_ref, 0, value + value.T)


EARLY_STREAMS = colored(EARLY_ROWS, ORDERS, 9)


def first_kernel(
    total, earlier_hbm, panels_hbm,
    top_hbm, low_hbm, flat_hbm, second_hbm, left_hbm, meet_hbm, out_hbm,
    second_ref, left_ref, meet_ref, out_ref, earlier, panels, turned, partial, sums, off, coeffs, near, mixed, top_all, low_all, flat_all, load, save, *scratch,
):
    ready = greet(ORDERS[0])
    scale = 1.0 / total
    chunks = earlier.shape[0] // 512
    loads = []
    for n in range(chunks):
        at = pl.ds(n * 512, 512)
        loads.append((
            pltpu.make_async_copy(earlier_hbm.at[at, :], earlier.at[at, :], load.at[0, n]),
            pltpu.make_async_copy(panels_hbm.at[at, :], panels.at[at, :], load.at[1, n]),
        ))
        for copy in loads[-1]:
            copy.start()
    for n in range(chunks):
        loads[n][0].wait()
        for i in range(4):
            turned[span(i), span(n, 512)] = earlier[span(n, 512), span(i)].T
    for n in range(chunks):
        loads[n][1].wait()

    @pl.loop(0, 4)
    def _(i):
        value = dot(turned[pl.ds(pl.multiple_of(i * PANEL, PANEL), PANEL), :], panels[...])
        for n in range(4):
            partial[pl.ds(pl.multiple_of(n * WIDTH + i * PANEL, PANEL), PANEL), :] = value[:, span(n, HALF)]

    scratch, sent = iter(scratch), []
    running = [stream(partial, sums, *one, scratch, sent) for one in EARLY_STREAMS]
    lead, rest = running[:4], running[4:]

    def gram_columns(j):
        for i in range(j + 1):
            put_slabs(partial, 4 * WIDTH + PAIRS.index((i, j)) * 512, dot(turned[span(i), :], earlier[:, span(j)]))

    ready()
    advance(lead)
    gram_columns(3)
    advance(lead)
    for j in range(3):
        gram_columns(j)
    advance(rest)
    for _ in range(7):
        advance(lead)
        advance(rest)

    for n in range(4):
        value = (sums[span(n, WIDTH), :] * scale).astype(BF16)
        coeffs[:WIDTH, span(n, HALF)] = value
        coeffs[WIDTH:, span(n, HALF)] = value

    @pl.loop(0, earlier.shape[0] // (2 * STEP))
    def _(n):
        for k in range(2):
            at = pl.ds(pl.multiple_of((2 * n + k) * STEP, STEP), STEP)
            flat = panels[at, :].astype(F32) - dot(earlier[at, :], coeffs[:WIDTH, :])
            top_all[at, :] = flat[:, :PANEL].astype(BF16)
            flat_all[at, :] = flat[:, PANEL:]

    saves = [pltpu.make_async_copy(flat_all, flat_hbm, save.at[0])]
    saves[0].start()
    advance(rest)

    for n, (i, j) in enumerate(PAIRS):
        block = read_slabs(sums, 4 * WIDTH + n * 512, PANEL, PANEL) * scale
        if i == j:
            rows = lax.broadcasted_iota(jnp.int32, block.shape, 0)
            columns = lax.broadcasted_iota(jnp.int32, block.shape, 1)
            block = block - (rows == columns).astype(F32)
        for k, value in enumerate(halves(block)):
            off[span(i), k * WIDTH + j * PANEL : k * WIDTH + (j + 1) * PANEL] = value
            if i != j:
                off[span(j), k * WIDTH + i * PANEL : k * WIDTH + (i + 1) * PANEL] = value.T
    beyond = dot(off[...], coeffs[...])
    for n in range(4):
        value = sums[span(n, WIDTH), :] * scale
        value = value - coeffs[:WIDTH, span(n, HALF)].astype(F32) - beyond[:, span(n, HALF)]
        if n < 2:
            near[:WIDTH, span(n, HALF)] = value.astype(BF16)
            near[WIDTH:, span(n, HALF)] = value.astype(BF16)
            left_ref[:, span(n, HALF)] = value - value.astype(BF16).astype(F32)
        else:
            second_ref[:, span(n - 2, HALF)] = value

    out_ref[...] = jnp.zeros_like(out_ref)
    mixed[...] = jnp.zeros_like(mixed)

    @pl.loop(0, earlier.shape[0] // (2 * STEP))
    def _(n):
        for k in range(2):
            at = pl.ds(pl.multiple_of((2 * n + k) * STEP, STEP), STEP)
            twice = top_all[at, :].astype(F32) - dot(earlier[at, :], near[:WIDTH, :])
            top, low = halves(twice)
            top_all[at, :] = top
            low_all[at, :] = low
            add_gram(top, low, panels[at, PANEL:], out_ref, mixed)

    saves += [pltpu.make_async_copy(top_all, top_hbm, save.at[1]), pltpu.make_async_copy(low_all, low_hbm, save.at[2])]
    saves[1].start()
    saves[2].start()
    close_gram(out_ref, mixed)
    saves.append(pltpu.make_async_copy(out_ref, out_hbm, save.at[3]))
    saves.append(pltpu.make_async_copy(second_ref, second_hbm, save.at[4]))
    for copy in saves[3:]:
        copy.start()
    left = left_ref[...] - dot(off[...], near[...])
    left_ref[...] = left
    left_t = left.T
    top, low = halves(left_t)
    meet_ref[...] = dot(top, coeffs[:WIDTH, PANEL:]) + dot(low, coeffs[:WIDTH, PANEL:])
    saves.append(pltpu.make_async_copy(left_ref, left_hbm, save.at[5]))
    saves.append(pltpu.make_async_copy(meet_ref, meet_hbm, save.at[6]))
    for copy in saves[5:]:
        copy.start()
    for copy in saves:
        copy.wait()
    for copy in sent:
        copy.wait_send()


def normalized(top, low, turned_top, turned_low):
    return (dot(top, turned_top) + (dot(top, turned_low) + dot(low, turned_top))).astype(BF16)


FIRST_STREAMS = [(0, FIRST_ROWS, ((G,), (X, Y), (Z,)))]
LAST_STREAMS = colored(LAST_ROWS, PLANES, 3)
SHIFT_AT = 512
AHEAD_AT = 1536


def second_kernel(
    total, part_hbm, left_hbm, second_hbm, meet_hbm, top_hbm, low_hbm, flat_hbm, earlier_hbm, later_hbm,
    basis_hbm, upper_hbm, newtop_hbm, newlow_hbm, last_hbm,
    part_ref, left_ref, second_ref, meet_ref, top_all, low_all, flat_all, earlier, later,
    basis, upper, sums, partial, last, work, inverse, turned_top, turned_low,
    fresh_b, near_e, near_q, mixed, load, save, *scratch,
):
    ready = greet([stage for _, _, stages in FIRST_STREAMS + LAST_STREAMS for stage in stages])
    scale = 1.0 / total
    loads = [
        pltpu.make_async_copy(src, dst, load.at[n])
        for n, (src, dst) in enumerate([
            (part_hbm, part_ref), (left_hbm, left_ref), (second_hbm, second_ref), (meet_hbm, meet_ref), (top_hbm, top_all),
            (low_hbm, low_all), (flat_hbm, flat_all), (earlier_hbm, earlier), (later_hbm, later),
        ])
    ]
    for copy in loads:
        copy.start()
    scratch, sent = iter(scratch), []
    running = [stream(part_ref, sums, *one, scratch, sent) for one in FIRST_STREAMS]
    ready()
    loads[0].wait()
    for _ in range(7):
        advance(running)
    for copy in loads[1:]:
        copy.wait()

    work[...] = read_slabs(sums, 0, PANEL, PANEL) * scale
    for _ in factor(work, upper, inverse):
        pass
    turn = inverse[...].T
    turned_top[...], turned_low[...] = halves(turn)
    fresh = exact(inverse[...], read_slabs(sums, 512, PANEL, PANEL) * scale)
    fresh_b[...] = fresh.astype(BF16)
    rounded = fresh.astype(BF16).astype(F32)
    near_q[...] = (fresh - rounded - exact(inverse[...], meet_ref[...])).astype(BF16)
    work[...] = exact(turn, rounded)

    @pl.loop(0, 4)
    def _(n):
        at = pl.ds(pl.multiple_of(n * PANEL, PANEL), PANEL)
        near_e[at, :] = (second_ref[at, :] - exact(left_ref[at, :], work[...])).astype(BF16)

    partial[...] = jnp.zeros_like(partial)
    mixed[...] = jnp.zeros_like(mixed)

    @pl.loop(0, earlier.shape[0] // STEP)
    def _(n):
        at = pl.ds(pl.multiple_of(n * STEP, STEP), STEP)
        newcols = normalized(top_all[at, :], low_all[at, :], turned_top[...], turned_low[...])
        basis[at, :] = newcols
        once = (flat_all[at, :] - dot(newcols, fresh_b[...])).astype(BF16)
        twice = once.astype(F32) - (dot(earlier[at, :], near_e[...]) + dot(newcols, near_q[...]))
        top, low = halves(twice)
        top_all[at, :] = top
        low_all[at, :] = low
        add_gram(top, low, None, partial, mixed)
        add_slabs(partial, SHIFT_AT, dot(newcols.T, later[at, :]))

    saves = [
        pltpu.make_async_copy(src, dst, save.at[n])
        for n, (src, dst) in enumerate([
            (basis, basis_hbm), (upper, upper_hbm), (top_all, newtop_hbm), (low_all, newlow_hbm), (last, last_hbm)
        ])
    ]
    for copy in saves[:4]:
        copy.start()
    close_gram(partial, mixed)
    running = [stream(partial, last, *one, scratch, sent) for one in LAST_STREAMS]
    lead, rest = running[:1], running[1:]
    advance(lead)

    @pl.loop(0, earlier.shape[0] // STEP)
    def _(n):
        at = pl.ds(pl.multiple_of(n * STEP, STEP), STEP)
        later_rows = later[at, :]
        add_slabs(partial, AHEAD_AT, dot(top_all[at, :].T, later_rows) + dot(low_all[at, :].T, later_rows))

    advance(lead)
    for _ in range(7):
        advance(rest)
        advance(lead)
    saves[4].start()
    for copy in saves:
        copy.wait()
    for copy in sent:
        copy.wait_send()


def third_kernel(
    total, sums_ref, first_upper_ref, first_ref, top_ref, low_ref, factors_ref, shift_ref, basis_ref,
    work, inverse, turned_top, turned_low,
):
    @pl.when(pl.program_id(0) == 0)
    def _():
        scale = 1.0 / total
        work[...] = read_slabs(sums_ref, 0, PANEL, PANEL) * scale
        factors_ref[0] = first_upper_ref[...]
        for _ in factor(work, factors_ref.at[1], inverse):
            pass
        turned_top[...], turned_low[...] = halves(inverse[...].T)
        shift_ref[:PANEL, :] = read_slabs(sums_ref, SHIFT_AT, PANEL, 512) * scale
        shift_ref[PANEL:, :] = exact(inverse[...], read_slabs(sums_ref, AHEAD_AT, PANEL, 512) * scale)

    basis_ref[:, :PANEL] = first_ref[...]
    basis_ref[:, PANEL:] = normalized(top_ref[...], low_ref[...], turned_top[...], turned_low[...])


def whole(*shape):
    return pl.BlockSpec(shape, lambda n: (0,) * len(shape))


def rows(columns):
    return pl.BlockSpec((2 * STEP, columns), lambda n: (n, 0))


def shape(*lengths, dtype=F32):
    return jax.ShapeDtypeStruct(lengths, dtype)


def body(earlier, snapshots, later):
    local = earlier.shape[0]
    total = local * lax.axis_size(AXES)
    square = pltpu.VMEM((PANEL, PANEL), F32)
    small = pltpu.VMEM((PANEL, PANEL), BF16)
    tall = pltpu.VMEM((WIDTH, PANEL), F32)
    outside = pl.BlockSpec(memory_space=pl.ANY)

    top, low, flat, second, left, meet, partial = pl.pallas_call(
        functools.partial(first_kernel, total),
        in_specs=[outside] * 2,
        out_specs=[outside] * 7,
        out_shape=[shape(local, PANEL, dtype=BF16), shape(local, PANEL, dtype=BF16), shape(local, PANEL),
                   shape(WIDTH, PANEL), shape(WIDTH, PANEL), shape(PANEL, PANEL), shape(FIRST_ROWS, HALF)],
        scratch_shapes=[tall, tall, square, pltpu.VMEM((FIRST_ROWS, HALF), F32),
                        pltpu.VMEM((local, WIDTH), BF16), pltpu.VMEM((local, 512), BF16), pltpu.VMEM((WIDTH, local), BF16),
                        pltpu.VMEM((EARLY_ROWS, HALF), F32), pltpu.VMEM((EARLY_ROWS, HALF), F32),
                        pltpu.VMEM((WIDTH, 2 * WIDTH), BF16), pltpu.VMEM((2 * WIDTH, 512), BF16),
                        pltpu.VMEM((2 * WIDTH, PANEL), BF16), square,
                        pltpu.VMEM((local, PANEL), BF16), pltpu.VMEM((local, PANEL), BF16), pltpu.VMEM((local, PANEL), F32),
                        pltpu.SemaphoreType.DMA((2, local // 512)), pltpu.SemaphoreType.DMA((7,))]
        + stream_scratch(EARLY_STREAMS),
        compiler_params=pltpu.CompilerParams(collective_id=1, has_side_effects=True, vmem_limit_bytes=62 * 2**20),
        name="first",
    )(earlier, snapshots)
    panel = pltpu.VMEM((local, PANEL), BF16)
    first, upper, top, low, last = pl.pallas_call(
        functools.partial(second_kernel, total),
        in_specs=[outside] * 9,
        out_specs=[outside] * 5,
        out_shape=[shape(local, PANEL, dtype=BF16), shape(PANEL, PANEL), shape(local, PANEL, dtype=BF16),
                   shape(local, PANEL, dtype=BF16), shape(LAST_ROWS, HALF)],
        scratch_shapes=[pltpu.VMEM((FIRST_ROWS, HALF), F32), tall, tall, square, panel, panel, pltpu.VMEM((local, PANEL), F32),
                        pltpu.VMEM((local, WIDTH), BF16), pltpu.VMEM((local, 512), BF16), panel, square,
                        pltpu.VMEM((FIRST_ROWS, HALF), F32), pltpu.VMEM((LAST_ROWS, HALF), F32), pltpu.VMEM((LAST_ROWS, HALF), F32),
                        square, square, small, small, small, pltpu.VMEM((WIDTH, PANEL), BF16), small, square,
                        pltpu.SemaphoreType.DMA((9,)), pltpu.SemaphoreType.DMA((5,))]
        + stream_scratch(FIRST_STREAMS + LAST_STREAMS),
        compiler_params=pltpu.CompilerParams(collective_id=2, has_side_effects=True, vmem_limit_bytes=60 * 2**20),
        name="second",
    )(partial, left, second, meet, top, low, flat, earlier, later)
    factors, shift_block, basis = pl.pallas_call(
        functools.partial(third_kernel, total),
        grid=(local // (2 * STEP),),
        in_specs=[whole(LAST_ROWS, HALF), whole(PANEL, PANEL), rows(PANEL), rows(PANEL), rows(PANEL)],
        out_specs=[whole(2, PANEL, PANEL), whole(512, 512), rows(512)],
        out_shape=[shape(2, PANEL, PANEL), shape(512, 512), shape(local, 512, dtype=BF16)],
        scratch_shapes=[square, square, small, small],
        compiler_params=pltpu.CompilerParams(dimension_semantics=("arbitrary",), vmem_limit_bytes=63 * 2**20),
        name="third",
    )(last, upper, first, top, low)
    return (basis, factors, shift_block)


def solution(mesh):
    torus = Mesh(mesh.devices.reshape(4, 4, 4, mesh.shape["grp"]), AXES)
    spec = P(AXES, None)
    return jax.shard_map(
        body, mesh=torus, in_specs=(spec, spec, spec), out_specs=(spec, P(), P()), check_vma=False
    )
```

```python
import functools
import itertools

import jax
import jax.numpy as jnp
from jax import lax
from jax.experimental import pallas as pl
from jax.experimental.pallas import tpu as pltpu
from jax.sharding import Mesh
from jax.sharding import PartitionSpec as P

PANEL = 256
BLOCK = 32
HALF = 128
F32 = jnp.float32
BF16 = jnp.bfloat16
MESH = pl.DeviceIdType.MESH
AXES = ("rows_0", "rows_1", "rows_2", "grp")


def thirds(value):
    top = value.astype(jnp.bfloat16)
    rest = value - top.astype(jnp.float32)
    middle = rest.astype(jnp.bfloat16)
    low = (rest - middle.astype(jnp.float32)).astype(jnp.bfloat16)
    return top, middle, low


def halves(value):
    top = value.astype(jnp.bfloat16)
    return top, (value - top.astype(jnp.float32)).astype(jnp.bfloat16)


def length_of(axis):
    return 2 if axis == "grp" or ":" in axis else 4


def size_of(stage):
    size = 1
    for axis in stage:
        size *= length_of(axis)
    return size


def offsets(stage):
    return [o for o in itertools.product(*[range(length_of(axis)) for axis in stage]) if any(o)]


def moved(axis, shift):
    name, _, pairing = axis.partition(":")
    at = lax.axis_index(name)
    if pairing == "a":
        return name, at + 1 - 2 * lax.rem(at, 2)
    if pairing == "b":
        return name, lax.rem(at + 3 + 2 * lax.rem(at, 2), 4)
    return name, lax.rem(at + shift, length_of(axis))


def part_of(axis, at):
    pairing = axis.partition(":")[2]
    if pairing == "a":
        return lax.rem((at + 1) // 2, 2)
    if pairing == "b":
        return at // 2
    return at


def peer_of(stage, offset):
    return dict(moved(axis, shift) for axis, shift in zip(stage, offset) if shift)


def place_in(stage, offset=None):
    place = 0
    for n, axis in enumerate(stage):
        at = moved(axis, offset[n])[1] if offset is not None and offset[n] else lax.axis_index(axis.partition(":")[0])
        place = place * length_of(axis) + part_of(axis, at)
    return place


def greet(stages):
    peers = []
    for stage in stages:
        for offset in offsets(stage):
            key = tuple(sorted((axis, shift) for axis, shift in zip(stage, offset) if shift))
            if key not in peers:
                peers.append(key)
    barrier = pltpu.get_barrier_semaphore()
    for key in peers:
        pl.semaphore_signal(
            barrier, inc=1, device_id=peer_of([a for a, _ in key], [n for _, n in key]), device_id_type=MESH
        )
    return lambda: pl.semaphore_wait(barrier, len(peers))


def levels_of(rows, stages):
    for stage in stages:
        rows //= size_of(stage)
        assert rows % 8 == 0
        yield stage, offsets(stage), rows


def stream_scratch(streams):
    shapes = []
    for _, rows, stages in streams:
        for stage, offs, length in levels_of(rows, stages):
            shapes += [pltpu.VMEM((len(offs), length, HALF), F32), pltpu.VMEM((length, HALF), F32)]
            shapes += [pltpu.SemaphoreType.DMA((len(offs),))] * 4
    return shapes


def copy_to(src, dst, send, recv, stage, offset):
    return pltpu.make_async_remote_copy(
        src_ref=src, dst_ref=dst, send_sem=send, recv_sem=recv, device_id=peer_of(stage, offset), device_id_type=MESH
    )


def stream(x_ref, o_ref, start, rows, stages, scratch, sent):
    levels = [level + tuple(next(scratch) for _ in range(6)) for level in levels_of(rows, stages)]
    where, src, base = start, x_ref, start
    for n, (stage, offs, length, slots, acc, send, recv, _, _) in enumerate(levels):
        copies = []
        for k, offset in enumerate(offs):
            at = pl.multiple_of(base + place_in(stage, offset) * length, 8)
            copies.append(copy_to(src.at[pl.ds(at, length), :], slots.at[k], send.at[k], recv.at[k], stage, offset))
            copies[-1].start()
        sent += copies
        yield
        own = place_in(stage) * length
        for copy in copies:
            copy.wait_recv()
        value = src[pl.ds(pl.multiple_of(base + own, 8), length), :]
        for k in range(len(offs)):
            value = value + slots[k]
        where = where + own
        if n + 1 < len(levels):
            acc[...] = value
        else:
            o_ref[pl.ds(pl.multiple_of(where, 8), length), :] = value
        src, base = acc, 0
    for stage, offs, length, _, _, _, _, send, recv in reversed(levels):
        piece = o_ref.at[pl.ds(pl.multiple_of(where, 8), length), :]
        copies = [copy_to(piece, piece, send.at[k], recv.at[k], stage, offset) for k, offset in enumerate(offs)]
        for copy in copies:
            copy.start()
        sent += copies
        yield
        for copy in copies:
            copy.wait_recv()
        where = where - place_in(stage) * length


def advance(streams):
    for one in streams:
        next(one, None)


G, X, Y, Z = "grp", "rows_2", "rows_1", "rows_0"
ORDERS = [((G,), (X,), (Y,), (Z,)), ((G,), (Y,), (Z,), (X,)), ((G,), (Z,), (X,), (Y,))]
PLANES = [((G,), (X,), (Y, Z)), ((G,), (Y,), (Z, X)), ((G,), (Z,), (X, Y))]
AT_ONCE = [((G,), (X, Y, Z))]


def colored(rows, orders, count):
    return [(n * rows // count, rows // count, orders[n % len(orders)]) for n in range(count)]


def factor(work, upper_ref, inverse_ref):
    lane = lax.broadcasted_iota(jnp.int32, (BLOCK, PANEL), 1)
    sub = lax.broadcasted_iota(jnp.int32, (BLOCK, HALF), 0)
    lane_half = lax.broadcasted_iota(jnp.int32, (BLOCK, HALF), 1)
    for k in range(PANEL // BLOCK):
        at = k * BLOCK
        rows = work[at : at + BLOCK, :]
        base = at // HALF * HALF
        off = at - base
        diag = rows[:, base : base + HALF]
        cols = [jnp.broadcast_to(diag[:, off + j : off + j + 1], (BLOCK, HALF)) for j in range(BLOCK)]
        eye = (lane_half == sub + off).astype(jnp.float32)
        wide = [rows[:, :HALF], rows[:, HALF:]]
        own = base // HALF
        inside = (lane_half >= off) & (lane_half < off + BLOCK)
        wide[own] = jnp.where(inside, eye, wide[own])
        scale = jnp.zeros((BLOCK, HALF), jnp.float32)
        for j in range(BLOCK):
            pivot = jnp.broadcast_to(cols[j][j : j + 1, :], (BLOCK, HALF))
            scale = jnp.where(sub == j, pivot, scale)
            if j == BLOCK - 1:
                break
            ratio = cols[j] * (1.0 / pivot)
            ratio = jnp.where(sub > j, ratio, 0.0)
            for m in range(j + 1, BLOCK):
                cols[m] = cols[m] - ratio * jnp.broadcast_to(cols[j][m : m + 1, :], (BLOCK, HALF))
            for h in range(2):
                wide[h] = wide[h] - ratio * jnp.broadcast_to(wide[h][j : j + 1, :], (BLOCK, HALF))
            diag = diag - ratio * jnp.broadcast_to(diag[j : j + 1, :], (BLOCK, HALF))
        scale = lax.rsqrt(scale)
        done = jnp.concatenate([wide[0] * scale, wide[1] * scale], axis=1)
        inverse_ref[at : at + BLOCK, :] = jnp.where(lane < at + BLOCK, done, 0.0)
        upper_ref[at : at + BLOCK, :] = jnp.where(lane >= at + BLOCK, done, 0.0)
        upper_ref[at : at + BLOCK, base : base + HALF] = jnp.where(
            inside & (lane_half - off >= sub), diag * scale, upper_ref[at : at + BLOCK, base : base + HALF]
        )
        if at + BLOCK < PANEL:
            a, b, c = thirds(done)
            right = jnp.concatenate([a, b, a, c, a, b], axis=0)
            left = jnp.concatenate([a, a, b, a, c, b], axis=0)
            prod = lax.dot_general(left.T[at + BLOCK :, :], right, (((1,), (0,)), ((), ())), preferred_element_type=jnp.float32)
            rest = work[at + BLOCK :, :]
            lanes = lax.broadcasted_iota(jnp.int32, rest.shape, 1)
            rest = jnp.where((lanes >= at) & (lanes < at + BLOCK), 0.0, rest)
            work[at + BLOCK :, :] = rest - prod
        yield


WIDTH = 1024
STEP = 1024
EARLY_ROWS = 9216
FIRST_ROWS = 1024
LAST_ROWS = 3072


def dot(left, right):
    return jnp.dot(left, right, preferred_element_type=F32)


def exact(left, right):
    return jnp.dot(left, right, precision=lax.Precision.HIGHEST, preferred_element_type=F32)


PAIRS = [(i, j) for j in range(4) for i in range(j + 1)]


def span(n, length=PANEL):
    return slice(n * length, (n + 1) * length)


def put_slabs(ref, at, value):
    rows = value.shape[0]
    for n in range(value.shape[1] // HALF):
        ref[at + n * rows : at + (n + 1) * rows, :] = value[:, span(n, HALF)]


def add_slabs(ref, at, value):
    rows = value.shape[0]
    for n in range(value.shape[1] // HALF):
        ref[at + n * rows : at + (n + 1) * rows, :] += value[:, span(n, HALF)]


def read_slabs(ref, at, rows, columns):
    return jnp.concatenate([ref[at + n * rows : at + (n + 1) * rows, :] for n in range(columns // HALF)], axis=1)


def add_gram(top, low, others, out_ref, mixed):
    top_t, low_t = top.T, low.T
    add_slabs(out_ref, 0, dot(top_t, top) + dot(low_t, low))
    mixed[...] += dot(top_t, low)
    if others is not None:
        add_slabs(out_ref, 512, dot(top_t, others) + dot(low_t, others))


def close_gram(out_ref, mixed):
    value = mixed[...]
    add_slabs(out_ref, 0, value + value.T)


EARLY_STREAMS = colored(EARLY_ROWS, ORDERS, 9)


def first_kernel(
    total, earlier_hbm, panels_hbm,
    top_hbm, low_hbm, flat_hbm, second_hbm, left_hbm, meet_hbm, out_hbm,
    second_ref, left_ref, meet_ref, out_ref, earlier, panels, turned, partial, sums, off, coeffs, near, mixed, top_all, low_all, flat_all, load, save, *scratch,
):
    ready = greet(ORDERS[0])
    scale = 1.0 / total
    chunks = earlier.shape[0] // 512
    loads = []
    for n in range(chunks):
        at = pl.ds(n * 512, 512)
        loads.append((
            pltpu.make_async_copy(earlier_hbm.at[at, :], earlier.at[at, :], load.at[0, n]),
            pltpu.make_async_copy(panels_hbm.at[at, :], panels.at[at, :], load.at[1, n]),
        ))
        for copy in loads[-1]:
            copy.start()
    for n in range(chunks):
        loads[n][0].wait()
        for i in range(4):
            turned[span(i), span(n, 512)] = earlier[span(n, 512), span(i)].T
    for n in range(chunks):
        loads[n][1].wait()

    @pl.loop(0, 4)
    def _(i):
        value = dot(turned[pl.ds(pl.multiple_of(i * PANEL, PANEL), PANEL), :], panels[...])
        for n in range(4):
            partial[pl.ds(pl.multiple_of(n * WIDTH + i * PANEL, PANEL), PANEL), :] = value[:, span(n, HALF)]

    scratch, sent = iter(scratch), []
    running = [stream(partial, sums, *one, scratch, sent) for one in EARLY_STREAMS]
    lead, rest = running[:4], running[4:]

    def gram_columns(j):
        for i in range(j + 1):
            put_slabs(partial, 4 * WIDTH + PAIRS.index((i, j)) * 512, dot(turned[span(i), :], earlier[:, span(j)]))

    ready()
    advance(lead)
    gram_columns(3)
    advance(lead)
    for j in range(3):
        gram_columns(j)
    advance(rest)
    for _ in range(6):
        advance(lead)
        advance(rest)
    advance(lead)

    for n in range(4):
        value = (sums[span(n, WIDTH), :] * scale).astype(BF16)
        coeffs[:WIDTH, span(n, HALF)] = value
        coeffs[WIDTH:, span(n, HALF)] = value

    @pl.loop(0, earlier.shape[0] // (2 * STEP))
    def _(n):
        at = pl.ds(pl.multiple_of(n * STEP, STEP), STEP)
        flat = panels[at, :].astype(F32) - dot(earlier[at, :], coeffs[:WIDTH, :])
        top_all[at, :] = flat[:, :PANEL].astype(BF16)
        flat_all[at, :] = flat[:, PANEL:]

    advance(rest)

    @pl.loop(earlier.shape[0] // (2 * STEP), earlier.shape[0] // STEP)
    def _(n):
        at = pl.ds(pl.multiple_of(n * STEP, STEP), STEP)
        flat = panels[at, :].astype(F32) - dot(earlier[at, :], coeffs[:WIDTH, :])
        top_all[at, :] = flat[:, :PANEL].astype(BF16)
        flat_all[at, :] = flat[:, PANEL:]

    saves = [pltpu.make_async_copy(flat_all, flat_hbm, save.at[0])]
    saves[0].start()
    advance(rest)

    for n, (i, j) in enumerate(PAIRS):
        block = read_slabs(sums, 4 * WIDTH + n * 512, PANEL, PANEL) * scale
        if i == j:
            rows = lax.broadcasted_iota(jnp.int32, block.shape, 0)
            columns = lax.broadcasted_iota(jnp.int32, block.shape, 1)
            block = block - (rows == columns).astype(F32)
        for k, value in enumerate(halves(block)):
            off[span(i), k * WIDTH + j * PANEL : k * WIDTH + (j + 1) * PANEL] = value
            if i != j:
                off[span(j), k * WIDTH + i * PANEL : k * WIDTH + (i + 1) * PANEL] = value.T
    beyond = dot(off[...], coeffs[...])
    for n in range(4):
        value = sums[span(n, WIDTH), :] * scale
        value = value - coeffs[:WIDTH, span(n, HALF)].astype(F32) - beyond[:, span(n, HALF)]
        if n < 2:
            near[:WIDTH, span(n, HALF)] = value.astype(BF16)
            near[WIDTH:, span(n, HALF)] = value.astype(BF16)
            left_ref[:, span(n, HALF)] = value - value.astype(BF16).astype(F32)
        else:
            second_ref[:, span(n - 2, HALF)] = value

    out_ref[...] = jnp.zeros_like(out_ref)
    mixed[...] = jnp.zeros_like(mixed)

    @pl.loop(0, earlier.shape[0] // (2 * STEP))
    def _(n):
        for k in range(2):
            at = pl.ds(pl.multiple_of((2 * n + k) * STEP, STEP), STEP)
            twice = top_all[at, :].astype(F32) - dot(earlier[at, :], near[:WIDTH, :])
            top, low = halves(twice)
            top_all[at, :] = top
            low_all[at, :] = low
            add_gram(top, low, panels[at, PANEL:], out_ref, mixed)

    saves += [pltpu.make_async_copy(top_all, top_hbm, save.at[1]), pltpu.make_async_copy(low_all, low_hbm, save.at[2])]
    saves[1].start()
    saves[2].start()
    close_gram(out_ref, mixed)
    saves.append(pltpu.make_async_copy(out_ref, out_hbm, save.at[3]))
    saves.append(pltpu.make_async_copy(second_ref, second_hbm, save.at[4]))
    for copy in saves[3:]:
        copy.start()
    left = left_ref[...] - dot(off[...], near[...])
    left_ref[...] = left
    left_t = left.T
    top, low = halves(left_t)
    meet_ref[...] = dot(top, coeffs[:WIDTH, PANEL:]) + dot(low, coeffs[:WIDTH, PANEL:])
    saves.append(pltpu.make_async_copy(left_ref, left_hbm, save.at[5]))
    saves.append(pltpu.make_async_copy(meet_ref, meet_hbm, save.at[6]))
    for copy in saves[5:]:
        copy.start()
    for copy in saves:
        copy.wait()
    for copy in sent:
        copy.wait_send()


def normalized(top, low, turned_top, turned_low):
    return (dot(top, turned_top) + (dot(top, turned_low) + dot(low, turned_top))).astype(BF16)


FIRST_STREAMS = [(0, FIRST_ROWS, ((G,), (X, Y), (Z,)))]
LAST_STREAMS = colored(LAST_ROWS, PLANES, 3)
SHIFT_AT = 512
AHEAD_AT = 1536


def second_kernel(
    total, part_hbm, left_hbm, second_hbm, meet_hbm, top_hbm, low_hbm, flat_hbm, earlier_hbm, later_hbm,
    basis_hbm, upper_hbm, newtop_hbm, newlow_hbm, last_hbm,
    part_ref, left_ref, second_ref, meet_ref, top_all, low_all, flat_all, earlier, later,
    basis, upper, sums, partial, last, work, inverse, turned_top, turned_low,
    fresh_b, near_e, near_q, mixed, load, save, *scratch,
):
    ready = greet([stage for _, _, stages in FIRST_STREAMS + LAST_STREAMS for stage in stages])
    scale = 1.0 / total
    loads = [
        pltpu.make_async_copy(src, dst, load.at[n])
        for n, (src, dst) in enumerate([
            (part_hbm, part_ref), (left_hbm, left_ref), (second_hbm, second_ref), (meet_hbm, meet_ref), (top_hbm, top_all),
            (low_hbm, low_all), (flat_hbm, flat_all), (earlier_hbm, earlier), (later_hbm, later),
        ])
    ]
    for copy in loads:
        copy.start()
    scratch, sent = iter(scratch), []
    running = [stream(part_ref, sums, *one, scratch, sent) for one in FIRST_STREAMS]
    ready()
    loads[0].wait()
    for _ in range(7):
        advance(running)
    for copy in loads[1:]:
        copy.wait()

    work[...] = read_slabs(sums, 0, PANEL, PANEL) * scale
    for _ in factor(work, upper, inverse):
        pass
    turn = inverse[...].T
    turned_top[...], turned_low[...] = halves(turn)
    fresh = exact(inverse[...], read_slabs(sums, 512, PANEL, PANEL) * scale)
    fresh_b[...] = fresh.astype(BF16)
    rounded = fresh.astype(BF16).astype(F32)
    near_q[...] = (fresh - rounded - exact(inverse[...], meet_ref[...])).astype(BF16)
    work[...] = exact(turn, rounded)

    @pl.loop(0, 4)
    def _(n):
        at = pl.ds(pl.multiple_of(n * PANEL, PANEL), PANEL)
        near_e[at, :] = (second_ref[at, :] - exact(left_ref[at, :], work[...])).astype(BF16)

    partial[...] = jnp.zeros_like(partial)
    mixed[...] = jnp.zeros_like(mixed)

    @pl.loop(0, earlier.shape[0] // STEP)
    def _(n):
        at = pl.ds(pl.multiple_of(n * STEP, STEP), STEP)
        newcols = normalized(top_all[at, :], low_all[at, :], turned_top[...], turned_low[...])
        basis[at, :] = newcols
        once = (flat_all[at, :] - dot(newcols, fresh_b[...])).astype(BF16)
        twice = once.astype(F32) - (dot(earlier[at, :], near_e[...]) + dot(newcols, near_q[...]))
        top, low = halves(twice)
        top_all[at, :] = top
        low_all[at, :] = low
        add_gram(top, low, None, partial, mixed)
        add_slabs(partial, SHIFT_AT, dot(newcols.T, later[at, :]))

    saves = [
        pltpu.make_async_copy(src, dst, save.at[n])
        for n, (src, dst) in enumerate([
            (basis, basis_hbm), (upper, upper_hbm), (top_all, newtop_hbm), (low_all, newlow_hbm), (last, last_hbm)
        ])
    ]
    for copy in saves[:4]:
        copy.start()
    close_gram(partial, mixed)
    running = [stream(partial, last, *one, scratch, sent) for one in LAST_STREAMS]
    lead, rest = running[:1], running[1:]
    advance(lead)

    @pl.loop(0, earlier.shape[0] // STEP)
    def _(n):
        at = pl.ds(pl.multiple_of(n * STEP, STEP), STEP)
        later_rows = later[at, :]
        add_slabs(partial, AHEAD_AT, dot(top_all[at, :].T, later_rows) + dot(low_all[at, :].T, later_rows))

    advance(lead)
    for _ in range(7):
        advance(rest)
        advance(lead)
    saves[4].start()
    for copy in saves:
        copy.wait()
    for copy in sent:
        copy.wait_send()


def third_kernel(
    total, sums_ref, first_upper_ref, first_ref, top_ref, low_ref, factors_ref, shift_ref, basis_ref,
    work, inverse, turned_top, turned_low,
):
    @pl.when(pl.program_id(0) == 0)
    def _():
        scale = 1.0 / total
        work[...] = read_slabs(sums_ref, 0, PANEL, PANEL) * scale
        factors_ref[0] = first_upper_ref[...]
        for _ in factor(work, factors_ref.at[1], inverse):
            pass
        turned_top[...], turned_low[...] = halves(inverse[...].T)
        shift_ref[:PANEL, :] = read_slabs(sums_ref, SHIFT_AT, PANEL, 512) * scale
        shift_ref[PANEL:, :] = exact(inverse[...], read_slabs(sums_ref, AHEAD_AT, PANEL, 512) * scale)

    basis_ref[:, :PANEL] = first_ref[...]
    basis_ref[:, PANEL:] = normalized(top_ref[...], low_ref[...], turned_top[...], turned_low[...])


def whole(*shape):
    return pl.BlockSpec(shape, lambda n: (0,) * len(shape))


def rows(columns):
    return pl.BlockSpec((2 * STEP, columns), lambda n: (n, 0))


def shape(*lengths, dtype=F32):
    return jax.ShapeDtypeStruct(lengths, dtype)


def body(earlier, snapshots, later):
    local = earlier.shape[0]
    total = local * lax.axis_size(AXES)
    square = pltpu.VMEM((PANEL, PANEL), F32)
    small = pltpu.VMEM((PANEL, PANEL), BF16)
    tall = pltpu.VMEM((WIDTH, PANEL), F32)
    outside = pl.BlockSpec(memory_space=pl.ANY)

    top, low, flat, second, left, meet, partial = pl.pallas_call(
        functools.partial(first_kernel, total),
        in_specs=[outside] * 2,
        out_specs=[outside] * 7,
        out_shape=[shape(local, PANEL, dtype=BF16), shape(local, PANEL, dtype=BF16), shape(local, PANEL),
                   shape(WIDTH, PANEL), shape(WIDTH, PANEL), shape(PANEL, PANEL), shape(FIRST_ROWS, HALF)],
        scratch_shapes=[tall, tall, square, pltpu.VMEM((FIRST_ROWS, HALF), F32),
                        pltpu.VMEM((local, WIDTH), BF16), pltpu.VMEM((local, 512), BF16), pltpu.VMEM((WIDTH, local), BF16),
                        pltpu.VMEM((EARLY_ROWS, HALF), F32), pltpu.VMEM((EARLY_ROWS, HALF), F32),
                        pltpu.VMEM((WIDTH, 2 * WIDTH), BF16), pltpu.VMEM((2 * WIDTH, 512), BF16),
                        pltpu.VMEM((2 * WIDTH, PANEL), BF16), square,
                        pltpu.VMEM((local, PANEL), BF16), pltpu.VMEM((local, PANEL), BF16), pltpu.VMEM((local, PANEL), F32),
                        pltpu.SemaphoreType.DMA((2, local // 512)), pltpu.SemaphoreType.DMA((7,))]
        + stream_scratch(EARLY_STREAMS),
        compiler_params=pltpu.CompilerParams(collective_id=1, has_side_effects=True, vmem_limit_bytes=62 * 2**20),
        name="first",
    )(earlier, snapshots)
    panel = pltpu.VMEM((local, PANEL), BF16)
    first, upper, top, low, last = pl.pallas_call(
        functools.partial(second_kernel, total),
        in_specs=[outside] * 9,
        out_specs=[outside] * 5,
        out_shape=[shape(local, PANEL, dtype=BF16), shape(PANEL, PANEL), shape(local, PANEL, dtype=BF16),
                   shape(local, PANEL, dtype=BF16), shape(LAST_ROWS, HALF)],
        scratch_shapes=[pltpu.VMEM((FIRST_ROWS, HALF), F32), tall, tall, square, panel, panel, pltpu.VMEM((local, PANEL), F32),
                        pltpu.VMEM((local, WIDTH), BF16), pltpu.VMEM((local, 512), BF16), panel, square,
                        pltpu.VMEM((FIRST_ROWS, HALF), F32), pltpu.VMEM((LAST_ROWS, HALF), F32), pltpu.VMEM((LAST_ROWS, HALF), F32),
                        square, square, small, small, small, pltpu.VMEM((WIDTH, PANEL), BF16), small, square,
                        pltpu.SemaphoreType.DMA((9,)), pltpu.SemaphoreType.DMA((5,))]
        + stream_scratch(FIRST_STREAMS + LAST_STREAMS),
        compiler_params=pltpu.CompilerParams(collective_id=2, has_side_effects=True, vmem_limit_bytes=60 * 2**20),
        name="second",
    )(partial, left, second, meet, top, low, flat, earlier, later)
    factors, shift_block, basis = pl.pallas_call(
        functools.partial(third_kernel, total),
        grid=(local // (2 * STEP),),
        in_specs=[whole(LAST_ROWS, HALF), whole(PANEL, PANEL), rows(PANEL), rows(PANEL), rows(PANEL)],
        out_specs=[whole(2, PANEL, PANEL), whole(512, 512), rows(512)],
        out_shape=[shape(2, PANEL, PANEL), shape(512, 512), shape(local, 512, dtype=BF16)],
        scratch_shapes=[square, square, small, small],
        compiler_params=pltpu.CompilerParams(dimension_semantics=("arbitrary",), vmem_limit_bytes=63 * 2**20),
        name="third",
    )(last, upper, first, top, low)
    return (basis, factors, shift_block)


def solution(mesh):
    torus = Mesh(mesh.devices.reshape(4, 4, 4, mesh.shape["grp"]), AXES)
    spec = P(AXES, None)
    return jax.shard_map(
        body, mesh=torus, in_specs=(spec, spec, spec), out_specs=(spec, P(), P()), check_vma=False
    )
```
